256 devices in a mesh: gx: 8 (over x, core), gy: 4 (over z_hi), gz: 8 (over z_lo, y).
Axes of the slice: x: 4, y: 4, z: 8 (z_hi: 4, z_lo: 2; z = z_hi * 2 + z_lo), core: 2. Of those that a mesh axis runs over, the one named last changes fastest.
Arguments:
- hidden_rows: bfloat16 [4096, 16384], P(('gx', 'gy'), 'gz'), may hold values from -2000 to 2000
- norm_gain: bfloat16 [16384], P('gz'), may hold values from 0.5 to 1.5
- w_query: bfloat16 [16384, 16384], P('gz', ('gx', 'gy')), may hold values from -0.046875 to 0.046875
- w_keyval: bfloat16 [16384, 2048], P('gz', ('gx', 'gy')), may hold values from -0.046875 to 0.046875
- positions: int32 [4096], P('gz'), may hold values from 0 to 1023, as said below
- keyval_order: int32 [8], replicated, may hold values from 0 to 7, each once
Outputs:
- queries: bfloat16 [4096, 16384], P('gz', ('gx', 'gy'))
- keyval_owned: bfloat16 [8, 4096, 256], P('gy', 'gz')
The draws below stay inside these ranges and needn't reach their ends.
Inputs may be any that keep to these rules, and one draw needn't show every extreme that they name: `positions`: each token's position within its packed document: 0 where a document starts, else one more than the previous token's; a document holds at most 1024 tokens. `keyval_order`: each head once.
All inputs are finite; a program needn't handle non-finite values.
Results may differ from the reference program's by a relative error of at most 0.0066.
Values may be sent and summed in bfloat16 or wider, within the bound.
A program may use at most 128 MiB of HBM per device.

```python
import math
import jax
import jax.numpy as jnp
from jax import lax

D = 16384
HQ = 128
KVH = 8
HD = 128
TOKENS = 4096


def draw_hidden_rows(key, part):
    key_rows, key_cols, key_base = jax.random.split(key, 3)
    row_scale = jnp.exp(jax.random.uniform(key_rows, (TOKENS, 1), jnp.float32, 0.0, math.log(10.0)))
    col_place = jnp.arange(D, dtype=jnp.float32) / D
    col_scale = jnp.exp(math.log(3.0) * col_place + jax.random.uniform(key_cols, (D,), jnp.float32, 0.0, math.log(10.0)))
    base_values = jnp.clip(jax.random.normal(key_base, (TOKENS, D), jnp.float32), -6.0, 6.0)
    scaled_values = jnp.clip(base_values * row_scale * col_scale[None, :], -2000.0, 2000.0)
    return scaled_values.astype(jnp.bfloat16)


def draw_positions(key, part):
    longest = TOKENS // 4
    spacing = min(512, max(4, longest // 2))
    marks = jax.random.randint(key, (TOKENS,), 0, spacing)
    index_all = jnp.arange(TOKENS, dtype=jnp.int32)
    is_start = (marks == 0) & (index_all >= longest) | (index_all % longest == 0)
    starts = jnp.where(is_start, index_all, 0)
    return (index_all - lax.cummax(starts, axis=0)).astype(jnp.int32)


def level_of(stream_key, shape, pieces, least, largest):
    def one(dim, blocks):
        draws = jax.random.uniform(jax.random.fold_in(jax.random.fold_in(stream_key, 6), dim), (blocks,), jnp.float32, least / len(pieces), largest / len(pieces))
        return jnp.repeat(jnp.exp(draws), shape[dim] // blocks).reshape((-1,) + (1,) * (len(shape) - dim - 1))

    factor_of = one(*pieces[0])
    for cut in pieces[1:]:
        factor_of = factor_of * one(*cut)
    return factor_of


def normal_values(stream_key, dims, deviation, limit, cuts=(), kind=jnp.bfloat16):
    entries = deviation * jax.random.normal(stream_key, dims, jnp.float32)
    if cuts:
        entries = entries * level_of(stream_key, dims, cuts, -0.22, 0.18)
    return jnp.clip(entries, -limit, limit).astype(kind)


def setup_inputs(seed: int = 0) -> dict:
    key_of = jax.random.split(jax.random.key(seed), 7)
    hidden_rows = draw_hidden_rows(jax.random.fold_in(key_of[6], 71), 0)
    norm_gain = jnp.clip(1.0 + 0.1 * jax.random.normal(key_of[1], (D,), jnp.float32), 0.5, 1.5).astype(jnp.bfloat16)
    w_query = normal_values(key_of[2], (D, HQ * HD), D ** -0.5, 0.046875, ((0, 8), (1, 32)))
    w_keyval = normal_values(key_of[3], (D, 2 * KVH * HD), D ** -0.5, 0.046875, ((0, 8), (1, 32)))
    positions = draw_positions(jax.random.fold_in(key_of[6], 71), 0)
    keyval_order = jax.random.permutation(key_of[5], KVH).astype(jnp.int32)
    return {"hidden_rows": hidden_rows, "norm_gain": norm_gain, "w_query": w_query, "w_keyval": w_keyval, "positions": positions, "keyval_order": keyval_order}


rope_base = 500000.0
norm_eps = 1e-05

def rotate_heads(values, position_ids):
    pair_index = jnp.arange(HD // 2, dtype=jnp.float32)
    inv_freq = jnp.exp(pair_index * (-2.0 * math.log(rope_base) / HD))
    angles = position_ids.astype(jnp.float32)[:, None] * inv_freq[None, :]
    cosines = jnp.cos(angles)[:, None, :]
    sine_part = jnp.sin(angles)[:, None, :]
    paired = values.reshape(values.shape[0], values.shape[1], HD // 2, 2)
    even_part = paired[..., 0]
    odd_part = paired[..., 1]
    rotated = jnp.stack([even_part * cosines - odd_part * sine_part, even_part * sine_part + odd_part * cosines], axis=-1)
    return rotated.reshape(values.shape)

def reference(hidden_rows, norm_gain, w_query, w_keyval, positions, keyval_order):
    widened = hidden_rows.astype(jnp.float32)
    mean_square = lax.optimization_barrier(jnp.sum(widened * widened, axis=1)) / D
    normed = (widened * lax.rsqrt(mean_square + norm_eps)[:, None] * norm_gain.astype(jnp.float32)).astype(jnp.bfloat16)
    query_raw = jnp.dot(normed, w_query, preferred_element_type=jnp.float32)
    queries = rotate_heads(query_raw.reshape(TOKENS, HQ, HD), positions).reshape(TOKENS, HQ * HD).astype(jnp.bfloat16)
    keyval_raw = jnp.dot(normed, w_keyval, preferred_element_type=jnp.float32).reshape(TOKENS, KVH, 2, HD)
    key_rot = rotate_heads(keyval_raw[:, :, 0, :], positions)
    keyval_rot = jnp.stack([key_rot, keyval_raw[:, :, 1, :]], axis=2).reshape(TOKENS, KVH, 2 * HD).astype(jnp.bfloat16)
    keyval_owned = jnp.transpose(keyval_rot[:, keyval_order, :], (1, 0, 2))
    return (queries, keyval_owned)
```

```python
import functools
import math

import jax
import jax.numpy as jnp
import numpy as np
from jax import lax
from jax.experimental import pallas as pl
from jax.experimental.pallas import tpu as pltpu
from jax.sharding import PartitionSpec as P

D = 16384
KVH = 8
HD = 128
rope_base = 500000.0
norm_eps = 1e-05

MESH = pl.DeviceIdType.MESH
F32 = jnp.float32
BF16 = jnp.bfloat16

O, L, R, F = 0, 3, 1, 2

STEPS = [
    ((O, O), []),
    ((L, O), [(L, O, 0), (R, O, 1), (L, O, 1), (R, O, 0), (O, L, 0), (O, R, 1)]),
    ((R, O), []),
    ((F, O), [(F, O, 0), (F, O, 1)]),
    ((O, L), [(O, L, 1), (O, R, 0)]),
    ((O, R), []),
    ((O, F), [(L, L, 0), (R, R, 1), (L, R, 1), (R, L, 0), (O, F, 0), (O, F, 1), (L, L, 1), (R, R, 0)]),
    ((L, L), [(L, R, 0), (R, L, 1)]),
    ((R, R), []),
    ((L, R), []),
    ((R, L), []),
    ((L, F), [(F, L, 0), (F, R, 1), (L, F, 0), (R, F, 1), (L, F, 1), (R, F, 0)]),
    ((R, F), []),
    ((F, L), [(F, R, 0), (F, L, 1)]),
    ((F, R), []),
    ((F, F), [(F, F, 0), (F, F, 1)]),
]
N_STEPS = len(STEPS)
LAG_RELAY, LAG_PLANE, LAG_OWNER = 2, 4, 6

KV_EVENTS = (
    [(O, L, 0), (O, R, 1), (L, O, 0), (R, O, 1), (O, L, 1), (O, R, 0), (L, O, 1), (R, O, 0), (O, F, 0), (O, F, 1)]
    + [(F, O, 0), (F, O, 1)]
    + [(L, L, 0), (R, R, 1), (L, R, 1), (R, L, 0), (L, L, 1), (R, R, 0), (L, R, 0), (R, L, 1)]
    + [(F, L, 0), (F, R, 1), (L, F, 0), (R, F, 1), (L, F, 1), (R, F, 0)]
    + [(F, R, 0), (F, L, 1), (F, F, 0), (F, F, 1)]
)


def lookup(t, values):
    return sum((t == k).astype(jnp.int32) * v for k, v in enumerate(values) if v)


def fused(
    h_hbm, gain_ref, wq_hbm, wkv_hbm, pos_ref, freq_ref, order_ref,
    q_ref, kv_ref,
    rows, wq, wkv, w, part, inbox, kvs, cosines, sines,
    load_sem, a_send, a_recv, a_side_send, a_side_recv,
    k_send, k_recv, k_side_send, k_side_recv, r_send, r_recv,
):
    gx, gy, gz = lax.axis_index("gx"), lax.axis_index("gy"), lax.axis_index("gz")
    x, core, zh = gx // 2, gx % 2, gy
    zl, y = gz // 4, gz % 4
    tok = rows.shape[2]
    kdim = rows.shape[3]
    n_q = wq.shape[1]
    n_kv = wkv.shape[1]
    n_all = w.shape[1]

    def at(xx, cc, zz, yy, ll):
        return (2 * xx + cc, zz, ll * 4 + yy)

    sibling = at(x, 1 - core, zh, y, zl)
    x_up = at((x + 1) % 4, core, zh, y, zl)
    x_down = at((x + 3) % 4, core, zh, y, zl)
    z_up = at(x, core, (zh + 1) % 4, y, zl)
    z_down = at(x, core, (zh + 3) % 4, y, zl)

    loads = [
        pltpu.make_async_copy(h_hbm, rows.at[gx, gy], load_sem.at[0]),
        pltpu.make_async_copy(wq_hbm, wq, load_sem.at[1]),
        pltpu.make_async_copy(wkv_hbm, wkv, load_sem.at[2]),
    ]
    for load in loads:
        load.start()

    barrier = pltpu.get_barrier_semaphore()
    peers = [
        sibling, x_up, x_down, z_up, z_down,
        at(x, core, zh, (y + 1) % 4, zl), at(x, core, zh, (y + 3) % 4, zl), at(x, core, zh, y, 1 - zl),
    ]
    for peer in peers:
        pl.semaphore_signal(barrier, inc=1, device_id=peer, device_id_type=MESH)

    class Gather:
        def __init__(self, buf, send, recv, side_send, side_recv):
            self.buf, self.send, self.recv = buf, send, recv
            self.side_send, self.side_recv = side_send, side_recv
            self.size = buf.shape[2] // 2
            self.sent = []

        def piece(self, ox, oz, p, cls=None):
            c = core if cls is None else cls
            return self.buf.at[2 * ((x + ox) % 4) + c, (zh + oz) % 4, pl.ds(p * self.size, self.size)]

        def copy(self, which, index, recv_at, target):
            ref = self.piece(*which)
            return pltpu.make_async_remote_copy(
                src_ref=ref, dst_ref=ref, send_sem=self.send.at[index], recv_sem=self.recv.at[recv_at],
                device_id=target, device_id_type=MESH,
            )

        def push(self, ox, oz, p, to_x, to_z, target):
            args = (ox, oz, p), len(self.sent), (to_x, to_z, p), target
            self.copy(*args).start()
            self.sent.append(args)

        def side(self, ox, oz, p, cls=None):
            ref = self.piece(ox, oz, p, cls)
            return pltpu.make_async_remote_copy(
                src_ref=ref, dst_ref=ref, send_sem=self.side_send.at[ox, oz, p],
                recv_sem=self.side_recv.at[ox, oz, p], device_id=sibling, device_id_type=MESH,
            )

        def spread_x(self, oz, p):
            self.push(O, oz, p, L, oz, x_up)
            self.push(O, oz, p, R, oz, x_down)

        def begin(self):
            for p in (0, 1):
                self.push(O, O, p, O, L, z_up)
                self.push(O, O, 1 - p, O, R, z_down)
                self.push(O, O, p, L, O, x_up)
                self.push(O, O, 1 - p, R, O, x_down)
            for p in (0, 1):
                self.side(O, O, p).start()

        def arrive(self, ox, oz, p):
            self.copy((ox, oz, p), 0, (ox, oz, p), x_up).wait_recv()
            if ox == O:
                if (oz, p) == (L, 0):
                    self.push(O, L, 0, O, F, z_up)
                if (oz, p) == (R, 1):
                    self.push(O, R, 1, O, F, z_down)
                self.spread_x(oz, p)
            if (ox, p) == (L, 0):
                self.push(L, oz, 0, F, oz, x_up)
            if (ox, p) == (R, 1):
                self.push(R, oz, 1, F, oz, x_down)
            self.side(ox, oz, p).start()

        def finish(self):
            for args in self.sent:
                self.copy(*args).wait_send()
            for ox in range(4):
                for oz in range(4):
                    for p in (0, 1):
                        self.side(ox, oz, p).wait_send()

    gather = Gather(rows, a_send, a_recv, a_side_send, a_side_recv)
    kv_gather = Gather(kvs, k_send, k_recv, k_side_send, k_side_recv)

    loads[0].wait()
    pl.semaphore_wait(barrier, len(peers))
    gather.begin()

    loads[1].wait()
    loads[2].wait()
    side_len = 128
    row_id = lax.broadcasted_iota(jnp.int32, (side_len, side_len), 0)
    lane = lax.broadcasted_iota(jnp.int32, (side_len, side_len), 1)

    def scale(i, carry):
        diagonal = jnp.where(row_id == lane, jnp.broadcast_to(gain_ref[pl.ds(i, 1), :], (side_len, side_len)), 0.0)
        diagonal = diagonal.astype(BF16)
        band = pl.ds(pl.multiple_of(i * side_len, side_len), side_len)
        w[band, 0:n_q] = jnp.dot(diagonal, wq[band, :], preferred_element_type=F32).astype(BF16)
        narrow = jnp.dot(diagonal, wkv[band, :], preferred_element_type=F32)
        w[band, n_q:n_all] = jnp.concatenate([narrow, jnp.zeros((side_len, n_all - n_q - n_kv), F32)], axis=1).astype(BF16)
        return carry

    lax.fori_loop(0, kdim // side_len, scale, 0)

    def tables(i, carry):
        spread = jnp.broadcast_to(pos_ref[pl.ds(i, 1), :].astype(F32), (side_len, side_len))
        angles = jnp.transpose(spread) * freq_ref[0:1, :]
        band = pl.ds(pl.multiple_of(i * side_len, side_len), side_len)
        cosines[band, :] = jnp.cos(angles)
        s = jnp.sin(angles)
        sines[band, :] = jnp.where(lane % 2 == 0, -s, s)
        return carry

    lax.fori_loop(0, pos_ref.shape[0], tables, 0)
    kvs[gx, gy] = jnp.zeros(kvs.shape[2:], BF16)

    def unit(t, c):
        xx = (x + lookup(t, [s[0][0] for s in STEPS])) % 4
        zz = (zh + lookup(t, [s[0][1] for s in STEPS])) % 4
        y_own = (2 * xx + c) % 4
        zl_own = xx // 2
        step = 1 if c else 3
        relay, far, direct = (y_own + step) % 4, (y_own + 2) % 4, (y_own + 4 - step) % 4
        return xx, zz, y_own, zl_own, relay, far, direct

    def reduce_copy(t, c, slot, target):
        return pltpu.make_async_remote_copy(
            src_ref=part.at[t, c], dst_ref=inbox.at[t, c, slot], send_sem=r_send.at[t, c],
            recv_sem=r_recv.at[t, c, slot], device_id=target, device_id_type=MESH,
        )

    def landed(t, c, slot):
        reduce_copy(t, c, slot, sibling).wait_recv()

    tile_lane = lax.broadcasted_iota(jnp.int32, (tok, 128), 1)

    def split_square(tile):
        rest = tile - tile.astype(BF16).astype(F32)
        return jnp.where(tile_lane == n_kv + 1, tile + pltpu.roll(rest, 1, 1), tile).astype(BF16)

    def add_up(t, c, slots):
        for n0 in range(0, n_q, 128):
            cols = pl.ds(n0, 128)
            total = part[t, c, :, cols].astype(F32)
            for slot in slots:
                total = total + inbox[t, c, slot, :, cols].astype(F32)
            part[t, c, :, cols] = total.astype(BF16)
        cols = pl.ds(n_q, 128)
        total = part[t, c, :, cols].astype(F32)
        for slot in slots:
            total = total + inbox[t, c, slot, :, cols].astype(F32)
        part[t, c, :, cols] = split_square(total)

    def compute(t):
        xx, zz = unit(t, 0)[:2]
        ox = lookup(t, [s[0][0] for s in STEPS])
        oz = lookup(t, [s[0][1] for s in STEPS])
        for p in (0, 1):
            gather.side(ox, oz, p, 1 - core).wait_recv()
        pair = pl.ds(2 * xx, 2)
        squares = jnp.zeros((2 * tok, 128), F32)
        for k0 in range(0, kdim, 128):
            some = rows[pair, zz, :, k0 : k0 + 128].reshape(2 * tok, 128).astype(F32)
            squares = squares + some * some
        square = jnp.sum(squares, axis=1, keepdims=True)
        high = square.astype(BF16).astype(F32)
        low = square - high
        lhs = rows[pair, zz].reshape(2 * tok, kdim)
        for n0 in range(0, n_q, 256):
            c_tile = jnp.dot(lhs, w[:, n0 : n0 + 256], preferred_element_type=F32).astype(BF16)
            part[t, 0, :, n0 : n0 + 256] = c_tile[:tok]
            part[t, 1, :, n0 : n0 + 256] = c_tile[tok:]
        last = jnp.dot(lhs, w[:, n_q:n_all], preferred_element_type=F32)
        wide = lax.broadcasted_iota(jnp.int32, (2 * tok, 128), 1)
        last = jnp.where(wide == n_kv, high, jnp.where(wide == n_kv + 1, low, last)).astype(BF16)
        part[t, 0, :, n_q:n_all] = last[:tok]
        part[t, 1, :, n_q:n_all] = last[tok:]
        for c in (0, 1):
            _, _, y_own, _, relay, far, direct = unit(t, c)

            @pl.when(y == far)
            def _():
                reduce_copy(t, c, 0, at(x, core, zh, relay, zl)).start()

            @pl.when(y == direct)
            def _():
                reduce_copy(t, c, 0, at(x, core, zh, y_own, zl)).start()

    def relay_stage(t):
        for c in (0, 1):
            _, _, y_own, _, relay, far, direct = unit(t, c)

            @pl.when(y == relay)
            def _():
                landed(t, c, 0)
                add_up(t, c, [0])
                reduce_copy(t, c, 1, at(x, core, zh, y_own, zl)).start()

    def plane_stage(t):
        for c in (0, 1):
            _, _, y_own, zl_own, relay, far, direct = unit(t, c)

            @pl.when((y == y_own) & (zl != zl_own))
            def _():
                landed(t, c, 0)
                landed(t, c, 1)
                add_up(t, c, [0, 1])
                reduce_copy(t, c, 2, at(x, core, zh, y, zl_own)).start()

    def rotate(tile, cos_t, sin_t):
        swapped = jnp.where(tile_lane % 2 == 0, pltpu.roll(tile, 127, 1), pltpu.roll(tile, 1, 1))
        return tile * cos_t + swapped * sin_t

    def owner_stage(t):
        for c in (0, 1):
            _, zz, y_own, zl_own, relay, far, direct = unit(t, c)

            @pl.when((y == y_own) & (zl == zl_own))
            def _():
                for slot in range(3):
                    landed(t, c, slot)

                def total(n0):
                    cols = pl.ds(n0, 128)
                    value = part[t, c, :, cols].astype(F32)
                    for slot in range(3):
                        value = value + inbox[t, c, slot, :, cols].astype(F32)
                    return value

                tail = total(n_q)
                square = jnp.sum(jnp.where((tile_lane == n_kv) | (tile_lane == n_kv + 1), tail, 0.0), axis=1, keepdims=True)
                factor = lax.rsqrt(square / D + norm_eps)
                band = pl.ds(pl.multiple_of(zz * tok, tok), tok)
                cos_t, sin_t = cosines[band, :], sines[band, :]
                for n0 in range(0, n_q, 128):
                    q_ref[band, n0 : n0 + 128] = rotate(total(n0) * factor, cos_t, sin_t).astype(BF16)
                tail = tail * factor
                odd = jnp.full((tok, 128), gy % 2, jnp.int32) == 1
                is_key = jnp.full((tok, 128), gy // 2, jnp.int32) == 0
                cos_k = jnp.where(odd, pltpu.roll(cos_t, 64, 1), cos_t)
                sin_k = jnp.where(odd, pltpu.roll(sin_t, 64, 1), sin_t)
                value = jnp.where(is_key, rotate(tail, cos_k, sin_k), tail)
                upper = jnp.full((tok, 128), zz // 2, jnp.int32)
                value = jnp.where(upper == 1, pltpu.roll(value, 64, 1), value)
                half = pl.ds(pl.multiple_of((zz % 2) * tok, tok), tok)
                old = kvs[gx, gy, half, :].astype(F32)
                kvs[gx, gy, half, :] = jnp.where(tile_lane // 64 == upper, value, old).astype(BF16)

    def step(t, carry):
        for k, (_, events) in enumerate(STEPS):
            if events:

                @pl.when(t == k)
                def _():
                    for event in events:
                        gather.arrive(*event)

        @pl.when(t < N_STEPS)
        def _():
            compute(t)

        @pl.when((t >= LAG_RELAY) & (t < N_STEPS + LAG_RELAY))
        def _():
            relay_stage(t - LAG_RELAY)

        @pl.when((t >= LAG_PLANE) & (t < N_STEPS + LAG_PLANE))
        def _():
            plane_stage(t - LAG_PLANE)

        @pl.when((t >= LAG_OWNER) & (t < N_STEPS + LAG_OWNER))
        def _():
            owner_stage(t - LAG_OWNER)

        return carry

    lax.fori_loop(0, N_STEPS + LAG_OWNER, step, 0)

    kv_gather.begin()
    for event in KV_EVENTS:
        kv_gather.arrive(*event)
    for ox in range(4):
        for oz in range(4):
            for p in (0, 1):
                kv_gather.side(ox, oz, p, 1 - core).wait_recv()
    slots = kv_ref.shape[0]
    half_rows = kvs.shape[2]
    half_lane = lax.broadcasted_iota(jnp.int32, (half_rows, 128), 1)
    for s in range(slots):
        head = order_ref[slots * gy + s]
        for g in (0, 1):
            first = kvs[head, 2 * g].astype(F32)
            second = kvs[head, 2 * g + 1].astype(F32)
            cols = slice(g * 128, g * 128 + 128)
            kv_ref[s, 0:half_rows, cols] = jnp.where(half_lane < 64, first, pltpu.roll(second, 64, 1)).astype(BF16)
            kv_ref[s, half_rows : 2 * half_rows, cols] = jnp.where(half_lane < 64, pltpu.roll(first, 64, 1), second).astype(BF16)

    gather.finish()
    kv_gather.finish()

    def drain(t, carry):
        for c in (0, 1):
            _, _, y_own, zl_own, relay, far, direct = unit(t, c)

            @pl.when((y != y_own) | (zl != zl_own))
            def _():
                reduce_copy(t, c, 0, sibling).wait_send()

        return carry

    lax.fori_loop(0, N_STEPS, drain, 0)


def body(hidden_rows, norm_gain, w_query, w_keyval, positions, keyval_order):
    tok, kdim = hidden_rows.shape
    n_q, n_kv = w_query.shape[1], w_keyval.shape[1]
    n_all = n_q + 128
    n_tok = positions.shape[0]
    freq = np.exp((np.arange(128) // 2) * (-2.0 * math.log(rope_base) / HD)).astype(np.float32)[None, :]
    hbm = pl.BlockSpec(memory_space=pl.ANY)
    vmem = pl.BlockSpec(memory_space=pltpu.VMEM)
    dma = pltpu.SemaphoreType.DMA
    return pl.pallas_call(
        fused,
        out_shape=(
            jax.ShapeDtypeStruct((n_tok, n_q), BF16),
            jax.ShapeDtypeStruct((2, n_tok, 2 * HD), BF16),
        ),
        in_specs=[hbm, vmem, hbm, hbm, vmem, vmem, pl.BlockSpec(memory_space=pltpu.SMEM)],
        out_specs=(vmem, vmem),
        scratch_shapes=[
            pltpu.VMEM((8, 4, tok, kdim), BF16),
            pltpu.VMEM((kdim, n_q), BF16),
            pltpu.VMEM((kdim, n_kv), BF16),
            pltpu.VMEM((kdim, n_all), BF16),
            pltpu.VMEM((N_STEPS, 2, tok, n_all), BF16),
            pltpu.VMEM((N_STEPS, 2, 3, tok, n_all), BF16),
            pltpu.VMEM((8, 4, n_tok // 2, 128), BF16),
            pltpu.VMEM((n_tok, 128), F32),
            pltpu.VMEM((n_tok, 128), F32),
            dma((3,)),
            dma((30,)), dma((4, 4, 2)), dma((4, 4, 2)), dma((4, 4, 2)),
            dma((30,)), dma((4, 4, 2)), dma((4, 4, 2)), dma((4, 4, 2)),
            dma((N_STEPS, 2)), dma((N_STEPS, 2, 3)),
        ],
        compiler_params=pltpu.CompilerParams(
            collective_id=0, has_side_effects=True, vmem_limit_bytes=62 * 1024 * 1024
        ),
        name="fused",
    )(
        hidden_rows,
        norm_gain.astype(F32).reshape(-1, 128),
        w_query,
        w_keyval,
        positions.reshape(-1, 128),
        jnp.asarray(freq),
        keyval_order,
    )


def solution(mesh):
    in_specs = (
        P(("gx", "gy"), "gz"),
        P("gz"),
        P("gz", ("gx", "gy")),
        P("gz", ("gx", "gy")),
        P("gz"),
        P(),
    )
    out_specs = (P("gz", ("gx", "gy")), P("gy", "gz", None))
    return jax.shard_map(body, mesh=mesh, in_specs=in_specs, out_specs=out_specs, check_vma=False)
```

```python
import functools
import math

import jax
import jax.numpy as jnp
import numpy as np
from jax import lax
from jax.experimental import pallas as pl
from jax.experimental.pallas import tpu as pltpu
from jax.sharding import PartitionSpec as P

D = 16384
KVH = 8
HD = 128
rope_base = 500000.0
norm_eps = 1e-05

MESH = pl.DeviceIdType.MESH
F32 = jnp.float32
BF16 = jnp.bfloat16

O, L, R, F = 0, 3, 1, 2

STEPS = [
    ((O, O), []),
    ((L, O), [(L, O, 0), (R, O, 1), (L, O, 1), (R, O, 0), (O, L, 0), (O, R, 1)]),
    ((R, O), []),
    ((F, O), [(F, O, 0), (F, O, 1)]),
    ((O, L), [(O, L, 1), (O, R, 0)]),
    ((O, R), []),
    ((O, F), [(L, L, 0), (R, R, 1), (L, R, 1), (R, L, 0), (O, F, 0), (O, F, 1), (L, L, 1), (R, R, 0)]),
    ((L, L), [(L, R, 0), (R, L, 1)]),
    ((R, R), []),
    ((L, R), []),
    ((R, L), []),
    ((L, F), [(F, L, 0), (F, R, 1), (L, F, 0), (R, F, 1), (L, F, 1), (R, F, 0)]),
    ((R, F), []),
    ((F, L), [(F, R, 0), (F, L, 1)]),
    ((F, R), []),
    ((F, F), [(F, F, 0), (F, F, 1)]),
]
N_STEPS = len(STEPS)
LAG_RELAY, LAG_PLANE, LAG_OWNER = 2, 4, 6

KV_EVENTS = (
    [(O, L, 0), (O, R, 1), (L, O, 0), (R, O, 1), (O, L, 1), (O, R, 0), (L, O, 1), (R, O, 0), (O, F, 0), (O, F, 1)]
    + [(F, O, 0), (F, O, 1)]
    + [(L, L, 0), (R, R, 1), (L, R, 1), (R, L, 0), (L, L, 1), (R, R, 0), (L, R, 0), (R, L, 1)]
    + [(F, L, 0), (F, R, 1), (L, F, 0), (R, F, 1), (L, F, 1), (R, F, 0)]
    + [(F, R, 0), (F, L, 1), (F, F, 0), (F, F, 1)]
)


def lookup(t, values):
    return sum((t == k).astype(jnp.int32) * v for k, v in enumerate(values) if v)


def fused(
    h_hbm, gain_ref, wq_hbm, wkv_hbm, pos_ref, freq_ref, order_ref,
    q_ref, kv_ref,
    rows, wq, wkv, w, part, part_kv, inbox, inbox_kv, kvs, factors, cosines, sines,
    load_sem, a_send, a_recv, a_side_send, a_side_recv,
    k_send, k_recv, k_side_send, k_side_recv, r_send, r_recv, r_kv_send, r_kv_recv,
):
    gx, gy, gz = lax.axis_index("gx"), lax.axis_index("gy"), lax.axis_index("gz")
    x, core, zh = gx // 2, gx % 2, gy
    zl, y = gz // 4, gz % 4
    tok = rows.shape[2]
    kdim = rows.shape[3]
    n_q = wq.shape[1]
    n_kv = wkv.shape[0]
    n_all = w.shape[1]

    def at(xx, cc, zz, yy, ll):
        return (2 * xx + cc, zz, ll * 4 + yy)

    sibling = at(x, 1 - core, zh, y, zl)
    x_up = at((x + 1) % 4, core, zh, y, zl)
    x_down = at((x + 3) % 4, core, zh, y, zl)
    z_up = at(x, core, (zh + 1) % 4, y, zl)
    z_down = at(x, core, (zh + 3) % 4, y, zl)

    loads = [
        pltpu.make_async_copy(h_hbm, rows.at[gx, gy], load_sem.at[0]),
        pltpu.make_async_copy(wq_hbm, wq, load_sem.at[1]),
        pltpu.make_async_copy(wkv_hbm, wkv, load_sem.at[2]),
    ]
    for load in loads:
        load.start()

    barrier = pltpu.get_barrier_semaphore()
    peers = [
        sibling, x_up, x_down, z_up, z_down,
        at(x, core, zh, (y + 1) % 4, zl), at(x, core, zh, (y + 3) % 4, zl), at(x, core, zh, y, 1 - zl),
    ]
    for peer in peers:
        pl.semaphore_signal(barrier, inc=1, device_id=peer, device_id_type=MESH)

    class Gather:
        def __init__(self, buf, send, recv, side_send, side_recv):
            self.buf, self.send, self.recv = buf, send, recv
            self.side_send, self.side_recv = side_send, side_recv
            self.size = buf.shape[2] // 2
            self.sent = []

        def piece(self, ox, oz, p, cls=None):
            c = core if cls is None else cls
            return self.buf.at[2 * ((x + ox) % 4) + c, (zh + oz) % 4, pl.ds(p * self.size, self.size)]

        def copy(self, which, index, recv_at, target):
            ref = self.piece(*which)
            return pltpu.make_async_remote_copy(
                src_ref=ref, dst_ref=ref, send_sem=self.send.at[index], recv_sem=self.recv.at[recv_at],
                device_id=target, device_id_type=MESH,
            )

        def push(self, ox, oz, p, to_x, to_z, target):
            args = (ox, oz, p), len(self.sent), (to_x, to_z, p), target
            self.copy(*args).start()
            self.sent.append(args)

        def side(self, ox, oz, p, cls=None):
            ref = self.piece(ox, oz, p, cls)
            return pltpu.make_async_remote_copy(
                src_ref=ref, dst_ref=ref, send_sem=self.side_send.at[ox, oz, p],
                recv_sem=self.side_recv.at[ox, oz, p], device_id=sibling, device_id_type=MESH,
            )

        def spread_x(self, oz, p):
            self.push(O, oz, p, L, oz, x_up)
            self.push(O, oz, p, R, oz, x_down)

        def begin(self):
            for p in (0, 1):
                self.push(O, O, p, O, L, z_up)
                self.push(O, O, 1 - p, O, R, z_down)
                self.push(O, O, p, L, O, x_up)
                self.push(O, O, 1 - p, R, O, x_down)
            for p in (0, 1):
                self.side(O, O, p).start()

        def arrive(self, ox, oz, p):
            self.copy((ox, oz, p), 0, (ox, oz, p), x_up).wait_recv()
            if ox == O:
                if (oz, p) == (L, 0):
                    self.push(O, L, 0, O, F, z_up)
                if (oz, p) == (R, 1):
                    self.push(O, R, 1, O, F, z_down)
                self.spread_x(oz, p)
            if (ox, p) == (L, 0):
                self.push(L, oz, 0, F, oz, x_up)
            if (ox, p) == (R, 1):
                self.push(R, oz, 1, F, oz, x_down)
            self.side(ox, oz, p).start()

        def finish(self):
            for args in self.sent:
                self.copy(*args).wait_send()
            for ox in range(4):
                for oz in range(4):
                    for p in (0, 1):
                        self.side(ox, oz, p).wait_send()

    gather = Gather(rows, a_send, a_recv, a_side_send, a_side_recv)
    kv_gather = Gather(kvs, k_send, k_recv, k_side_send, k_side_recv)

    loads[0].wait()
    pl.semaphore_wait(barrier, len(peers))
    gather.begin()

    loads[1].wait()
    loads[2].wait()
    side_len = 128
    row_id = lax.broadcasted_iota(jnp.int32, (side_len, side_len), 0)
    lane = lax.broadcasted_iota(jnp.int32, (side_len, side_len), 1)

    for i in range(kdim // side_len):
        band = slice(i * side_len, (i + 1) * side_len)
        gain = jnp.broadcast_to(gain_ref[:, band].astype(F32), (side_len, side_len))
        diagonal = jnp.where(row_id == lane, gain, 0.0).astype(BF16)
        w[band, 0:n_q] = jnp.dot(diagonal, wq[band, :], preferred_element_type=F32).astype(BF16)
        narrow = lax.dot_general(diagonal, wkv[:, band], (((1,), (1,)), ((), ())), preferred_element_type=F32)
        w[band, n_q:n_all] = jnp.concatenate([narrow, jnp.zeros((side_len, n_all - n_q - n_kv), F32)], axis=1).astype(BF16)

    def tables(i, carry):
        spread = jnp.broadcast_to(pos_ref[pl.ds(i, 1), :].astype(F32), (side_len, side_len))
        angles = jnp.transpose(spread) * freq_ref[0:1, :]
        band = pl.ds(pl.multiple_of(i * side_len, side_len), side_len)
        cosines[band, :] = jnp.cos(angles)
        s = jnp.sin(angles)
        sines[band, :] = jnp.where(lane % 2 == 0, -s, s)
        return carry

    lax.fori_loop(0, pos_ref.shape[0], tables, 0)
    kvs[gx, gy] = jnp.zeros(kvs.shape[2:], BF16)

    def unit(t, c):
        xx = (x + lookup(t, [s[0][0] for s in STEPS])) % 4
        zz = (zh + lookup(t, [s[0][1] for s in STEPS])) % 4
        y_own = (2 * xx + c) % 4
        zl_own = xx // 2
        step = 1 if c else 3
        relay, far, direct = (y_own + step) % 4, (y_own + 2) % 4, (y_own + 4 - step) % 4
        return xx, zz, y_own, zl_own, relay, far, direct

    class Reduction:
        def __init__(self, part, inbox, send, recv):
            self.part, self.inbox, self.send, self.recv = part, inbox, send, recv

        def copy(self, t, c, slot, target):
            return pltpu.make_async_remote_copy(
                src_ref=self.part.at[t, c], dst_ref=self.inbox.at[t, c, slot], send_sem=self.send.at[t, c],
                recv_sem=self.recv.at[t, c, slot], device_id=target, device_id_type=MESH,
            )

        def landed(self, t, c, slot):
            self.copy(t, c, slot, sibling).wait_recv()

        def total(self, t, c, slots, cols):
            value = self.part[t, c, :, cols].astype(F32)
            for slot in slots:
                value = value + self.inbox[t, c, slot, :, cols].astype(F32)
            return value

        def first(self, t):
            for c in (0, 1):
                _, _, y_own, _, relay, far, direct = unit(t, c)

                @pl.when(y == far)
                def _():
                    self.copy(t, c, 0, at(x, core, zh, relay, zl)).start()

                @pl.when(y == direct)
                def _():
                    self.copy(t, c, 0, at(x, core, zh, y_own, zl)).start()

        def relay(self, t):
            for c in (0, 1):
                _, _, y_own, _, relay, far, direct = unit(t, c)

                @pl.when(y == relay)
                def _():
                    self.landed(t, c, 0)
                    self.add_up(t, c, [0])
                    self.copy(t, c, 1, at(x, core, zh, y_own, zl)).start()

        def plane(self, t):
            for c in (0, 1):
                _, _, y_own, zl_own, relay, far, direct = unit(t, c)

                @pl.when((y == y_own) & (zl != zl_own))
                def _():
                    self.landed(t, c, 0)
                    self.landed(t, c, 1)
                    self.add_up(t, c, [0, 1])
                    self.copy(t, c, 2, at(x, core, zh, y, zl_own)).start()

        def owner(self, t):
            for c in (0, 1):
                _, zz, y_own, zl_own, relay, far, direct = unit(t, c)

                @pl.when((y == y_own) & (zl == zl_own))
                def _():
                    for slot in range(3):
                        self.landed(t, c, slot)
                    self.store(t, c, zz)

        def drain(self, t):
            for c in (0, 1):
                _, _, y_own, zl_own, relay, far, direct = unit(t, c)

                @pl.when((y != y_own) | (zl != zl_own))
                def _():
                    self.copy(t, c, 0, sibling).wait_send()

    tile_lane = lax.broadcasted_iota(jnp.int32, (tok, 128), 1)

    def rotate(tile, cos_t, sin_t):
        swapped = jnp.where(tile_lane % 2 == 0, pltpu.roll(tile, 127, 1), pltpu.roll(tile, 1, 1))
        return tile * cos_t + swapped * sin_t

    class QueryReduction(Reduction):
        def add_up(self, t, c, slots):
            for n0 in range(0, n_q, 128):
                cols = slice(n0, n0 + 128)
                self.part[t, c, :, cols] = self.total(t, c, slots, cols).astype(BF16)

        def store(self, t, c, zz):
            band = pl.ds(pl.multiple_of(zz * tok, tok), tok)
            factor, cos_t, sin_t = factors[band, :], cosines[band, :], sines[band, :]
            for n0 in range(0, n_q, 128):
                cols = slice(n0, n0 + 128)
                value = self.total(t, c, range(3), cols) * factor
                q_ref[band, cols] = rotate(value, cos_t, sin_t).astype(BF16)

    class KeyValueReduction(Reduction):
        def add_up(self, t, c, slots):
            tile = self.total(t, c, slots, slice(0, 128))
            rest = tile - tile.astype(BF16).astype(F32)
            tile = jnp.where(tile_lane == n_kv + 1, tile + pltpu.roll(rest, 1, 1), tile)
            self.part[t, c] = tile.astype(BF16)

        def store(self, t, c, zz):
            band = pl.ds(pl.multiple_of(zz * tok, tok), tok)
            tile = self.total(t, c, range(3), slice(0, 128))
            is_square = (tile_lane == n_kv) | (tile_lane == n_kv + 1)
            square = jnp.sum(jnp.where(is_square, tile, 0.0), axis=1, keepdims=True)
            factor = jnp.broadcast_to(lax.rsqrt(square / D + norm_eps), (tok, 128))
            factors[band, :] = factor
            tile = tile * factor
            cos_t, sin_t = cosines[band, :], sines[band, :]
            odd = jnp.full((tok, 128), gy % 2, jnp.int32) == 1
            is_key = jnp.full((tok, 128), gy // 2, jnp.int32) == 0
            cos_t = jnp.where(odd, pltpu.roll(cos_t, 64, 1), cos_t)
            sin_t = jnp.where(odd, pltpu.roll(sin_t, 64, 1), sin_t)
            tile = jnp.where(is_key, rotate(tile, cos_t, sin_t), tile)
            upper = jnp.full((tok, 128), zz // 2, jnp.int32)
            tile = jnp.where(upper == 1, pltpu.roll(tile, 64, 1), tile)
            half = pl.ds(pl.multiple_of((zz % 2) * tok, tok), tok)
            old = kvs[gx, gy, half, :].astype(F32)
            kvs[gx, gy, half, :] = jnp.where(tile_lane // 64 == upper, tile, old).astype(BF16)

    query = QueryReduction(part, inbox, r_send, r_recv)
    keyval = KeyValueReduction(part_kv, inbox_kv, r_kv_send, r_kv_recv)

    def compute(t):
        xx, zz = unit(t, 0)[:2]
        ox = lookup(t, [s[0][0] for s in STEPS])
        oz = lookup(t, [s[0][1] for s in STEPS])
        for p in (0, 1):
            gather.side(ox, oz, p, 1 - core).wait_recv()
        pair = pl.ds(2 * xx, 2)
        squares = jnp.zeros((2 * tok, 128), F32)
        for k0 in range(0, kdim, 128):
            some = rows[pair, zz, :, k0 : k0 + 128].reshape(2 * tok, 128).astype(F32)
            squares = squares + some * some
        square = jnp.sum(squares, axis=1, keepdims=True)
        high = square.astype(BF16).astype(F32)
        low = square - high
        lhs = rows[pair, zz].reshape(2 * tok, kdim)
        last = jnp.dot(lhs, w[:, n_q:n_all], preferred_element_type=F32)
        wide = lax.broadcasted_iota(jnp.int32, (2 * tok, 128), 1)
        last = jnp.where(wide == n_kv, high, jnp.where(wide == n_kv + 1, low, last)).astype(BF16)
        part_kv[t, 0] = last[:tok]
        part_kv[t, 1] = last[tok:]
        keyval.first(t)
        for n0 in range(0, n_q, 256):
            c_tile = jnp.dot(lhs, w[:, n0 : n0 + 256], preferred_element_type=F32).astype(BF16)
            part[t, 0, :, n0 : n0 + 256] = c_tile[:tok]
            part[t, 1, :, n0 : n0 + 256] = c_tile[tok:]
        query.first(t)

    def step(t, carry):
        for k, (_, events) in enumerate(STEPS):
            if events:

                @pl.when(t == k)
                def _():
                    for event in events:
                        gather.arrive(*event)

        compute(t)
        for lag, stage in (
            (LAG_RELAY, "relay"), (LAG_PLANE, "plane"), (LAG_OWNER, "owner"),
        ):

            @pl.when(t >= lag)
            def _():
                getattr(keyval, stage)(t - lag)
                getattr(query, stage)(t - lag)

        return carry

    lax.fori_loop(0, N_STEPS, step, 0)

    def stages(stage, begin, end=N_STEPS):
        lax.fori_loop(begin, end, lambda t, carry: (stage(t), carry)[1], 0)

    stages(keyval.relay, N_STEPS - LAG_RELAY)
    stages(query.relay, N_STEPS - LAG_RELAY)
    stages(keyval.plane, N_STEPS - LAG_PLANE)
    stages(keyval.owner, N_STEPS - LAG_OWNER)
    kv_gather.begin()
    stages(query.plane, N_STEPS - LAG_PLANE, N_STEPS - 2)
    for event in KV_EVENTS[:8]:
        kv_gather.arrive(*event)
    stages(query.plane, N_STEPS - 2)
    for event in KV_EVENTS[8:20]:
        kv_gather.arrive(*event)
    stages(query.owner, N_STEPS - LAG_OWNER, N_STEPS - 2)
    for event in KV_EVENTS[20:]:
        kv_gather.arrive(*event)
    stages(query.owner, N_STEPS - 2)
    for ox in range(4):
        for oz in range(4):
            for p in (0, 1):
                kv_gather.side(ox, oz, p, 1 - core).wait_recv()
    slots = kv_ref.shape[0]
    half_rows = kvs.shape[2]
    half_lane = lax.broadcasted_iota(jnp.int32, (half_rows, 128), 1)
    for s in range(slots):
        head = order_ref[slots * gy + s]
        for g in (0, 1):
            first = kvs[head, 2 * g].astype(F32)
            second = kvs[head, 2 * g + 1].astype(F32)
            cols = slice(g * 128, g * 128 + 128)
            kv_ref[s, 0:half_rows, cols] = jnp.where(half_lane < 64, first, pltpu.roll(second, 64, 1)).astype(BF16)
            kv_ref[s, half_rows : 2 * half_rows, cols] = jnp.where(half_lane < 64, pltpu.roll(first, 64, 1), second).astype(BF16)

    gather.finish()
    kv_gather.finish()

    stages(keyval.drain, 0)
    stages(query.drain, 0)


def pass_on(q_in, kv_in, q_out, kv_out, q_buf, kv_buf, sems):
    takes, puts = [], []
    for n, (source, buf, target) in enumerate(((q_in, q_buf, q_out), (kv_in, kv_buf, kv_out))):
        half = buf.shape[0] // 2
        for i in (0, 1):
            piece = pl.ds(i * half, half)
            takes.append(pltpu.make_async_copy(source.at[piece], buf.at[piece], sems.at[0, n, i]))
            puts.append(pltpu.make_async_copy(buf.at[piece], target.at[piece], sems.at[1, n, i]))
    for take in takes:
        take.start()
    for take, put in zip(takes, puts):
        take.wait()
        put.start()
    for put in puts:
        put.wait()


def body(hidden_rows, norm_gain, w_query, w_keyval, positions, keyval_order):
    tok, kdim = hidden_rows.shape
    n_q, n_kv = w_query.shape[1], w_keyval.shape[1]
    n_all = n_q + 128
    n_tok = positions.shape[0]
    freq = np.exp((np.arange(128) // 2) * (-2.0 * math.log(rope_base) / HD)).astype(np.float32)[None, :]
    hbm = pl.BlockSpec(memory_space=pl.ANY)
    vmem = pl.BlockSpec(memory_space=pltpu.VMEM)
    dma = pltpu.SemaphoreType.DMA
    outs = (
        jax.ShapeDtypeStruct((n_tok, n_q), BF16),
        jax.ShapeDtypeStruct((2, n_tok, 2 * HD), BF16),
    )
    results = pl.pallas_call(
        fused,
        out_shape=outs,
        in_specs=[hbm, vmem, hbm, hbm, vmem, vmem, pl.BlockSpec(memory_space=pltpu.SMEM)],
        out_specs=(vmem, vmem),
        scratch_shapes=[
            pltpu.VMEM((8, 4, tok, kdim), BF16),
            pltpu.VMEM((kdim, n_q), BF16),
            pltpu.VMEM((n_kv, kdim), BF16),
            pltpu.VMEM((kdim, n_all), BF16),
            pltpu.VMEM((N_STEPS, 2, tok, n_q), BF16),
            pltpu.VMEM((N_STEPS, 2, tok, 128), BF16),
            pltpu.VMEM((N_STEPS, 2, 3, tok, n_q), BF16),
            pltpu.VMEM((N_STEPS, 2, 3, tok, 128), BF16),
            pltpu.VMEM((8, 4, n_tok // 2, 128), BF16),
            pltpu.VMEM((n_tok, 128), F32),
            pltpu.VMEM((n_tok, 128), F32),
            pltpu.VMEM((n_tok, 128), F32),
            dma((3,)),
            dma((30,)), dma((4, 4, 2)), dma((4, 4, 2)), dma((4, 4, 2)),
            dma((30,)), dma((4, 4, 2)), dma((4, 4, 2)), dma((4, 4, 2)),
            dma((N_STEPS, 2)), dma((N_STEPS, 2, 3)),
            dma((N_STEPS, 2)), dma((N_STEPS, 2, 3)),
        ],
        compiler_params=pltpu.CompilerParams(
            collective_id=0, has_side_effects=True, vmem_limit_bytes=62 * 1024 * 1024
        ),
        name="fused",
    )(
        hidden_rows,
        norm_gain.reshape(1, -1),
        w_query,
        w_keyval.T,
        positions.reshape(-1, 128),
        jnp.asarray(freq),
        keyval_order,
    )
    return pl.pallas_call(
        pass_on,
        out_shape=outs,
        in_specs=[hbm, hbm],
        out_specs=(hbm, hbm),
        scratch_shapes=[pltpu.VMEM(out.shape, out.dtype) for out in outs] + [dma((2, 2, 2))],
        name="pass_on",
    )(*results)


def solution(mesh):
    in_specs = (
        P(("gx", "gy"), "gz"),
        P("gz"),
        P("gz", ("gx", "gy")),
        P("gz", ("gx", "gy")),
        P("gz"),
        P(),
    )
    out_specs = (P("gz", ("gx", "gy")), P("gy", "gz", None))
    return jax.shard_map(body, mesh=mesh, in_specs=in_specs, out_specs=out_specs, check_vma=False)
```

```python
import functools
import math

import jax
import jax.numpy as jnp
import numpy as np
from jax import lax
from jax.experimental import pallas as pl
from jax.experimental.pallas import tpu as pltpu
from jax.sharding import PartitionSpec as P

D = 16384
KVH = 8
HD = 128
rope_base = 500000.0
norm_eps = 1e-05

MESH = pl.DeviceIdType.MESH
F32 = jnp.float32
BF16 = jnp.bfloat16

O, L, R, F = 0, 3, 1, 2

ARRIVALS = [
    [],
    [(L, O, 0), (R, O, 1)],
    [(L, O, 1), (R, O, 0)],
    [(O, L, 0), (O, R, 1), "weights_own"],
    [(F, O, 0), (F, O, 1)],
    [(L, L, 0), (R, R, 1)],
    [(O, L, 1), (O, R, 0)],
    [(L, R, 1), (R, L, 0)],
    [(L, L, 1), (R, R, 0)],
    [(O, F, 0), (O, F, 1)],
    [(L, R, 0), (R, L, 1)],
    ["weights_near", (F, L, 0), (F, R, 1)],
    [(L, F, 0), (R, F, 1)],
    ["weights_far", "kv_products", (L, F, 1), (R, F, 0)],
    ["kv_relay", (F, R, 0), (F, L, 1)],
    ["kv_plane", (F, F, 0), (F, F, 1)],
]
STEPS = [(O, O, 0), (O, O, 1)] + [e for events in ARRIVALS for e in events if not isinstance(e, str)]
N_STEPS = len(STEPS)
PAIR = {step: n // 2 for n, step in enumerate(STEPS)}

SLOTS = [(events, 2 * n + 2, max(2 * n - 2, 0), max(2 * n - 6, 0)) for n, events in enumerate(ARRIVALS)] + [
    (["kv_owner"], 32, 32, 28),
    (["kv_near"], 32, 32, 32),
    (["kv_far"], 32, 32, 32),
]
KV_STEPS = (O, L, R, F)

KV_EVENTS = [
    [(O, L, 0), (O, R, 1)], [(L, O, 0), (R, O, 1)], [(O, L, 1), (O, R, 0)], [(L, O, 1), (R, O, 0)], [(O, F, 0), (O, F, 1)],
    [(F, O, 0), (F, O, 1)], [(L, L, 0), (R, R, 1)], [(L, R, 1), (R, L, 0)], [(L, L, 1), (R, R, 0)], [(L, R, 0), (R, L, 1)],
    [(F, L, 0), (F, R, 1)], [(L, F, 0), (R, F, 1)], [(L, F, 1), (R, F, 0)], [(F, R, 0), (F, L, 1)], [(F, F, 0), (F, F, 1)],
]


def lookup(t, values):
    return sum((t == k).astype(jnp.int32) * v for k, v in enumerate(values) if v)


def fused(
    h_hbm, gain_ref, wq_hbm, wkv_hbm, pos_ref, freq_ref, order_ref,
    q_hbm, kv_hbm,
    rows, wq, w, wkv, w_kv, part, part_kv, inbox, inbox_kv, kvs, factors, cosines, sines,
    load_sem, a_send, a_recv, a_side_send, a_side_recv,
    k_send, k_recv, k_side_send, k_side_recv, r_send, r_recv, r_kv_send, r_kv_recv,
    w_send, w_recv, q_ref, kv_ref, out_sem,
):
    gx, gy, gz = lax.axis_index("gx"), lax.axis_index("gy"), lax.axis_index("gz")
    x, core, zh = gx // 2, gx % 2, gy
    zl, y = gz // 4, gz % 4
    tok = rows.shape[2]
    part_tok = tok // 2
    kdim = rows.shape[3]
    n_q = wq.shape[1]
    n_kv = wkv.shape[1]
    n_head = 4 * n_kv

    def at(xx, cc, zz, yy, ll):
        return (2 * xx + cc, zz, ll * 4 + yy)

    sibling = at(x, 1 - core, zh, y, zl)
    x_up = at((x + 1) % 4, core, zh, y, zl)
    x_down = at((x + 3) % 4, core, zh, y, zl)
    z_up = at(x, core, (zh + 1) % 4, y, zl)
    z_down = at(x, core, (zh + 3) % 4, y, zl)

    loads = [
        pltpu.make_async_copy(h_hbm, rows.at[gx, gy], load_sem.at[0]),
        pltpu.make_async_copy(wq_hbm, wq, load_sem.at[1]),
        pltpu.make_async_copy(wkv_hbm, wkv.at[gy], load_sem.at[2]),
    ]
    for load in loads:
        load.start()

    barrier = pltpu.get_barrier_semaphore()
    peers = [
        sibling, x_up, x_down, z_up, z_down,
        at(x, core, zh, (y + 1) % 4, zl), at(x, core, zh, (y + 3) % 4, zl), at(x, core, zh, y, 1 - zl),
    ]
    for peer in peers:
        pl.semaphore_signal(barrier, inc=1, device_id=peer, device_id_type=MESH)

    class Gather:
        def __init__(self, buf, sends, recv, side_send, side_recv):
            self.buf, self.sends, self.recv = buf, sends, recv
            self.side_send, self.side_recv = side_send, side_recv
            self.size, self.extra = tok // 2, buf.shape[2] - tok

        def piece(self, ox, oz, p, whole=False):
            size = self.size + (self.extra if whole and p else 0)
            return self.buf.at[2 * ((x + ox) % 4) + core, (zh + oz) % 4, pl.ds(p * self.size, size)]

        def push(self, ox, oz, p, to_x, to_z, target):
            along_z = to_x == O
            ref = self.piece(ox, oz, p, whole=along_z)
            pltpu.make_async_remote_copy(
                src_ref=ref, dst_ref=ref, send_sem=self.sends.at[int(along_z)],
                recv_sem=self.recv.at[PAIR[to_x, to_z, p]], device_id=target, device_id_type=MESH,
            ).start()

        def side(self, ox, oz, p):
            ref = self.piece(ox, oz, p)
            n = PAIR[ox, oz, p] if self.side_recv.shape[0] > 1 else 0
            pltpu.make_async_remote_copy(
                src_ref=ref, dst_ref=ref, send_sem=self.side_send, recv_sem=self.side_recv.at[n],
                device_id=sibling, device_id_type=MESH,
            ).start()

        def begin(self):
            for p in (0, 1):
                self.push(O, O, p, O, L, z_up)
                self.push(O, O, 1 - p, O, R, z_down)
                self.push(O, O, p, L, O, x_up)
                self.push(O, O, 1 - p, R, O, x_down)
            for p in (0, 1):
                self.side(O, O, p)

        def arrive(self, *pieces):
            whole = self.buf.at[0, 0] if pieces[0][0] == O else self.buf.at[0, 0, pl.ds(0, tok)]
            received(whole, self.recv.at[PAIR[pieces[0]]])
            if (O, L, 0) in pieces:
                self.push(O, L, 0, O, F, z_up)
            if (O, R, 1) in pieces:
                self.push(O, R, 1, O, F, z_down)
            for ox, oz, p in pieces:
                if ox == O:
                    self.push(O, oz, p, L, oz, x_up)
                if (ox, p) == (L, 0):
                    self.push(L, oz, 0, F, oz, x_up)
            for ox, oz, p in pieces[::-1]:
                if ox == O:
                    self.push(O, oz, p, R, oz, x_down)
                if (ox, p) == (R, 1):
                    self.push(R, oz, 1, F, oz, x_down)
            for piece in pieces:
                self.side(*piece)

        def finish(self):
            left(self.buf.at[pl.ds(0, 8), pl.ds(0, 3), pl.ds(0, self.size)], self.sends.at[0])
            left(self.buf.at[0, pl.ds(0, 3)], self.sends.at[1])
            left(self.buf.at[:, :, pl.ds(0, self.size)], self.side_send)

    def received(ref, sem):
        pltpu.make_async_remote_copy(
            src_ref=ref, dst_ref=ref, send_sem=a_side_send, recv_sem=sem, device_id=sibling, device_id_type=MESH
        ).wait_recv()

    def left(ref, sem):
        pltpu.make_async_remote_copy(
            src_ref=ref, dst_ref=ref, send_sem=sem, recv_sem=a_recv.at[0], device_id=sibling, device_id_type=MESH
        ).wait_send()

    gather = Gather(rows, a_send, a_recv, a_side_send, a_side_recv)
    kv_gather = Gather(kvs, k_send, k_recv, k_side_send, k_side_recv)

    half_kv = n_kv // 2

    def weights_copy(oz, p, to_z, target):
        ref = wkv.at[(zh + oz) % 4, pl.ds(p * half_kv, half_kv)]
        return pltpu.make_async_remote_copy(
            src_ref=ref, dst_ref=ref, send_sem=w_send, recv_sem=w_recv.at[0 if (to_z, p) in ((L, 0), (R, 1)) else 1],
            device_id=target, device_id_type=MESH,
        )

    weights_sent = [
        (O, 0, L, z_up), (O, 1, R, z_down), (O, 1, L, z_up), (O, 0, R, z_down),
        (L, 0, F, z_up), (R, 1, F, z_down),
    ]

    def weights_own():
        for args in weights_sent[:4]:
            weights_copy(*args).start()

    def weights_near():
        received(wkv.at[0], w_recv.at[0])
        for args in weights_sent[4:]:
            weights_copy(*args).start()

    def weights_far():
        received(wkv.at[pl.ds(0, 2)], w_recv.at[1])
        for g in range(4):
            w_kv[g * n_kv : (g + 1) * n_kv, :] = (wkv[g].astype(F32) * gain_ref[...].astype(F32)).astype(BF16)

    loads[0].wait()
    loads[2].wait()
    pl.semaphore_wait(barrier, len(peers))
    gather.begin()

    loads[1].wait()
    side_len = 128
    row_id = lax.broadcasted_iota(jnp.int32, (side_len, side_len), 0)
    lane = lax.broadcasted_iota(jnp.int32, (side_len, side_len), 1)

    for i in range(kdim // side_len):
        band = slice(i * side_len, (i + 1) * side_len)
        gain = jnp.broadcast_to(gain_ref[:, band].astype(F32), (side_len, side_len))
        diagonal = jnp.where(row_id == lane, gain, 0.0).astype(BF16)
        w[band, 0:n_q] = jnp.dot(diagonal, wq[band, :], preferred_element_type=F32).astype(BF16)

    def tables(i, carry):
        spread = jnp.broadcast_to(pos_ref[pl.ds(i, 1), :].astype(F32), (side_len, side_len))
        angles = jnp.transpose(spread) * freq_ref[0:1, :]
        band = pl.ds(pl.multiple_of(i * side_len, side_len), side_len)
        cosines[band, :] = jnp.cos(angles)
        s = jnp.sin(angles)
        sines[band, :] = jnp.where(lane % 2 == 0, -s, s)
        return carry

    lax.fori_loop(0, pos_ref.shape[0], tables, 0)

    def unit(t, xx, c):
        y_own = (2 * xx + c) % 4
        zl_own = xx // 2
        step = 1 + 2 * ((t + c) % 2)
        relay, far, direct = (y_own + step) % 4, (y_own + 2) % 4, (y_own + 4 - step) % 4
        return y_own, zl_own, relay, far, direct

    class Reduction:
        def __init__(self, part, inbox, send, recv):
            self.part, self.inbox, self.send, self.recv = part, inbox, send, recv

        def copy(self, t, c, slot, target):
            return pltpu.make_async_remote_copy(
                src_ref=self.own(t, c), dst_ref=self.inbox.at[t, c, slot], send_sem=self.send,
                recv_sem=self.recv.at[t, c], device_id=target, device_id_type=MESH,
            )

        def landed(self, t, c, count):
            received(self.inbox.at[t, c, pl.ds(0, count)], self.recv.at[t, c])

        def total(self, t, c, slots, band, cols):
            value = self.own(t, c)[band, cols].astype(F32)
            for slot in slots:
                value = value + self.inbox[t, c, slot, band, cols].astype(F32)
            return value

        def first(self, t):
            for c in (0, 1):
                y_own, _, relay, far, direct = unit(t, self.place(t)[0], c)

                @pl.when(y == far)
                def _():
                    self.copy(t, c, 0, at(x, core, zh, relay, zl)).start()

                @pl.when(y == direct)
                def _():
                    self.copy(t, c, 0, at(x, core, zh, y_own, zl)).start()

        def relay(self, t):
            for c in (0, 1):
                y_own, _, relay, far, direct = unit(t, self.place(t)[0], c)

                @pl.when(y == relay)
                def _():
                    self.landed(t, c, 1)
                    self.add_up(t, c, [0])
                    self.copy(t, c, 1, at(x, core, zh, y_own, zl)).start()

        def plane(self, t):
            for c in (0, 1):
                y_own, zl_own, relay, far, direct = unit(t, self.place(t)[0], c)

                @pl.when((y == y_own) & (zl != zl_own))
                def _():
                    self.landed(t, c, 2)
                    self.add_up(t, c, [0, 1])
                    self.copy(t, c, 2, at(x, core, zh, y, zl_own)).start()

        def owner(self, t):
            for c in (0, 1):
                xx, zz = self.place(t)
                y_own, zl_own, relay, far, direct = unit(t, xx, c)

                @pl.when((y == y_own) & (zl == zl_own))
                def _():
                    self.landed(t, c, 3)
                    self.store(t, c, zz)

    tile_lane = lax.broadcasted_iota(jnp.int32, (tok, 128), 1)
    short_row = lax.broadcasted_iota(jnp.int32, (16, 128), 0)

    def rotate(tile, cos_t, sin_t):
        swapped = jnp.where(tile_lane[: tile.shape[0]] % 2 == 0, pltpu.roll(tile, 127, 1), pltpu.roll(tile, 1, 1))
        return tile * cos_t + swapped * sin_t

    class QueryReduction(Reduction):
        def place(self, t):
            return (x + lookup(t, [s[0] for s in STEPS])) % 4, (zh + lookup(t, [s[1] for s in STEPS])) % 4

        def own(self, t, c):
            return self.part.at[t, c]

        def rows_of(self, t):
            return lookup(t, [s[2] for s in STEPS]) * part_tok

        def add_up(self, t, c, slots):
            for n0 in range(0, n_q, 128):
                cols = slice(n0, n0 + 128)
                self.own(t, c)[:, cols] = self.total(t, c, slots, slice(None), cols).astype(BF16)

        def store(self, t, c, zz):
            band = pl.ds(pl.multiple_of(zz * tok + self.rows_of(t), part_tok), part_tok)
            cos_t, sin_t, factor = cosines[band, :], sines[band, :], factors[band, :]
            for n0 in range(0, n_q, 128):
                cols = slice(n0, n0 + 128)
                value = self.total(t, c, range(3), slice(None), cols) * factor
                q_ref[band, cols] = rotate(value, cos_t, sin_t).astype(BF16)

    class KeyValueReduction(Reduction):
        def place(self, k):
            return (x + lookup(k, KV_STEPS)) % 4, zh

        def own(self, k, c):
            return self.part.at[2 * k + c]

        def add_up(self, t, c, slots):
            tile = self.total(t, c, slots, pl.ds(tok, 16), slice(0, 128))
            rest = tile - tile.astype(BF16).astype(F32)
            tile = jnp.where(short_row == 1, tile + pltpu.roll(rest, 1, 0), tile)
            self.own(t, c)[tok : tok + 16, 0:128] = tile.astype(BF16)
            for n0 in range(0, n_head, 128):
                cols = slice(n0, n0 + 128)
                self.own(t, c)[0:tok, cols] = self.total(t, c, slots, pl.ds(0, tok), cols).astype(BF16)

        def store(self, t, c, zz):
            band = pl.ds(pl.multiple_of(zz * tok, tok), tok)
            tile = self.total(t, c, range(3), pl.ds(tok, 16), slice(0, 128))
            square = jnp.sum(jnp.where(short_row < 2, tile, 0.0), axis=0, keepdims=True)
            factor = lax.rsqrt(square / D + norm_eps)
            first = factor.astype(BF16).astype(F32)
            second = (factor - first).astype(BF16).astype(F32)
            third = factor - first - second
            spread = jnp.where(short_row == 0, first, jnp.where(short_row == 1, second, third))
            kvs[gx, gy, tok : tok + 16, 0:128] = spread.astype(BF16)
            kvs[gx, gy, tok : tok + 16, 128:256] = jnp.zeros((16, 128), BF16)
            factor = jnp.transpose(jnp.broadcast_to(factor, (tok, 128)))
            everything = pl.ds(0, tok)
            key = self.total(t, c, range(3), everything, slice(0, 128)) * factor
            kvs[gx, gy, 0:tok, 0:128] = rotate(key, cosines[band, :], sines[band, :]).astype(BF16)
            value = self.total(t, c, range(3), everything, slice(128, 256)) * factor
            kvs[gx, gy, 0:tok, 128:256] = value.astype(BF16)

    query = QueryReduction(part, inbox, r_send, r_recv)
    keyval = KeyValueReduction(part_kv, inbox_kv, r_kv_send, r_kv_recv)

    def compute(t):
        xx, zz = query.place(t)
        p = lookup(t, [s[2] for s in STEPS])
        band = pl.ds(pl.multiple_of(p * part_tok, part_tok), part_tok)
        lhs = rows[pl.ds(2 * xx, 2), zz, band].reshape(tok, kdim)
        for n0 in range(0, n_q, 256):
            c_tile = jnp.dot(lhs, w[:, n0 : n0 + 256], preferred_element_type=F32).astype(BF16)
            part[t, 0, :, n0 : n0 + 256] = c_tile[:part_tok]
            part[t, 1, :, n0 : n0 + 256] = c_tile[part_tok:]
        query.first(t)

    def spread_factor(zz):
        pieces = kvs[gx, zz, tok : tok + 16, 0:128].astype(F32)
        factor = jnp.sum(jnp.where(short_row < 3, pieces, 0.0), axis=0, keepdims=True)
        band = pl.ds(pl.multiple_of(zz * tok, tok), tok)
        factors[band, :] = jnp.transpose(jnp.broadcast_to(factor, (tok, 128)))

    wide_lane = lax.broadcasted_iota(jnp.int32, (2 * tok, 128), 1)

    def kv_product(k):
        xx, zz = keyval.place(k)
        pair = pl.ds(2 * xx, 2)
        squares = jnp.zeros((2 * tok, 128), F32)
        for k0 in range(0, kdim, 128):
            some = rows[pair, zz, :, k0 : k0 + 128].reshape(2 * tok, 128).astype(F32)
            squares = squares + some * some
        square = jnp.sum(squares, axis=1, keepdims=True)
        high = square.astype(BF16).astype(F32)
        spread = jnp.where(wide_lane == 0, high, jnp.where(wide_lane == 1, square - high, 0.0))
        lhs = rows[pair, zz].reshape(2 * tok, kdim)
        tile = lax.dot_general(lhs, w_kv[...], (((1,), (1,)), ((), ())), preferred_element_type=F32).astype(BF16)
        for c in (0, 1):
            part_kv[2 * k + c, 0:tok, :] = tile[c * tok : (c + 1) * tok]
            turned = jnp.transpose(spread[c * tok : (c + 1) * tok])
            part_kv[2 * k + c, tok : tok + 16, 0:128] = turned[0:16].astype(BF16)
            part_kv[2 * k + c, tok : tok + 16, 128:256] = jnp.zeros((16, 128), BF16)
        keyval.first(k)

    def stages(stage, begin, end=N_STEPS):
        lax.fori_loop(begin, end, lambda t, carry: (stage(t), carry)[1], 0)

    named = {
        "kv_near": lambda: [kv_gather.arrive(*pieces) for pieces in KV_EVENTS[:4]],
        "kv_far": lambda: [kv_gather.arrive(*pieces) for pieces in KV_EVENTS[4:5]],
        "weights_near": weights_near,
        "weights_far": weights_far,
        "kv_products": lambda: stages(kv_product, 0, 4),
        "kv_relay": lambda: stages(keyval.relay, 0, 4),
        "kv_owner": lambda: (stages(keyval.owner, 0, 4), kv_gather.begin()),
        "kv_plane": lambda: stages(keyval.plane, 0, 4),
    }

    def slot(n, carry):
        for k, (events, _, _, _) in enumerate(SLOTS):
            if events:

                @pl.when(n == k)
                def _():
                    for event in events:
                        if isinstance(event, str) and event != "weights_own":
                            named[event]()
                    pieces = [event for event in events if not isinstance(event, str)]
                    if pieces:
                        gather.arrive(*pieces)
                    if "weights_own" in events:
                        weights_own()

        @pl.when(n < N_STEPS // 2)
        def _():
            received(rows.at[0, 0], a_side_recv.at[n])

        for at_slot, stage in ((1, compute), (2, query.relay), (3, query.plane)):
            counts = [s[at_slot] for s in SLOTS]
            stages(stage, lookup(n, [0] + counts[:-1]), lookup(n, counts))
        return carry

    lax.fori_loop(0, len(SLOTS), slot, 0)

    for event in KV_EVENTS[5:12]:
        kv_gather.arrive(*event)
    stages(spread_factor, 0, 4)
    stages(query.owner, 0)
    q_out = pltpu.make_async_copy(q_ref, q_hbm, out_sem.at[0])
    q_out.start()
    for event in KV_EVENTS[12:]:
        kv_gather.arrive(*event)
    received(kvs.at[:, :, pl.ds(0, tok // 2)], k_side_recv.at[0])
    slots = kv_ref.shape[0]
    for s in range(slots):
        head = order_ref[slots * gy + s]
        for g in range(4):
            kv_ref[s, g * tok : (g + 1) * tok, :] = kvs[head, g, 0:tok, :]
    kv_out = pltpu.make_async_copy(kv_ref, kv_hbm, out_sem.at[1])
    kv_out.start()

    gather.finish()
    kv_gather.finish()

    left(wkv.at[pl.ds(0, 3)], w_send)
    owned = N_STEPS // 4
    left(part.at[pl.ds(0, N_STEPS - owned // 2)], r_send)
    left(part_kv.at[pl.ds(0, 7)], r_kv_send)
    q_out.wait()
    kv_out.wait()


def pass_on(q_in, kv_in, q_out, kv_out, q_buf, kv_buf, sems):
    takes, puts = [], []
    for n, (source, buf, target) in enumerate(((q_in, q_buf, q_out), (kv_in, kv_buf, kv_out))):
        half = buf.shape[0] // 2
        for i in (0, 1):
            piece = pl.ds(i * half, half)
            takes.append(pltpu.make_async_copy(source.at[piece], buf.at[piece], sems.at[0, n, i]))
            puts.append(pltpu.make_async_copy(buf.at[piece], target.at[piece], sems.at[1, n, i]))
    for take in takes:
        take.start()
    for take, put in zip(takes, puts):
        take.wait()
        put.start()
    for put in puts:
        put.wait()


def body(hidden_rows, norm_gain, w_query, w_keyval, positions, keyval_order):
    tok, kdim = hidden_rows.shape
    n_q, n_kv = w_query.shape[1], w_keyval.shape[1]
    n_head = 4 * n_kv
    n_tok = positions.shape[0]
    freq = np.exp((np.arange(128) // 2) * (-2.0 * math.log(rope_base) / HD)).astype(np.float32)[None, :]
    hbm = pl.BlockSpec(memory_space=pl.ANY)
    vmem = pl.BlockSpec(memory_space=pltpu.VMEM)
    dma = pltpu.SemaphoreType.DMA
    outs = (
        jax.ShapeDtypeStruct((n_tok, n_q), BF16),
        jax.ShapeDtypeStruct((2, n_tok, 2 * HD), BF16),
    )
    results = pl.pallas_call(
        fused,
        out_shape=outs,
        in_specs=[hbm, vmem, hbm, hbm, vmem, vmem, pl.BlockSpec(memory_space=pltpu.SMEM)],
        out_specs=(hbm, hbm),
        scratch_shapes=[
            pltpu.VMEM((8, 4, tok, kdim), BF16),
            pltpu.VMEM((kdim, n_q), BF16),
            pltpu.VMEM((kdim, n_q), BF16),
            pltpu.VMEM((4, n_kv, kdim), BF16),
            pltpu.VMEM((n_head, kdim), BF16),
            pltpu.VMEM((N_STEPS, 2, tok // 2, n_q), BF16),
            pltpu.VMEM((8, tok + 16, n_head), BF16),
            pltpu.VMEM((N_STEPS, 2, 3, tok // 2, n_q), BF16),
            pltpu.VMEM((4, 2, 3, tok + 16, n_head), BF16),
            pltpu.VMEM((8, 4, tok + 16, n_head), BF16),
            pltpu.VMEM((n_tok, 128), F32),
            pltpu.VMEM((n_tok, 128), F32),
            pltpu.VMEM((n_tok, 128), F32),
            dma((3,)),
            dma((2,)), dma((N_STEPS // 2,)), dma(()), dma((N_STEPS // 2,)),
            dma((2,)), dma((N_STEPS // 2,)), dma(()), dma((1,)),
            dma(()), dma((N_STEPS, 2)), dma(()), dma((4, 2)),
            dma(()), dma((2,)),
            pltpu.VMEM((n_tok, n_q), BF16),
            pltpu.VMEM((2, n_tok, 2 * HD), BF16),
            dma((2,)),
        ],
        compiler_params=pltpu.CompilerParams(
            collective_id=0, has_side_effects=True, vmem_limit_bytes=62 * 1024 * 1024
        ),
        name="fused",
    )(
        hidden_rows,
        norm_gain.reshape(1, -1),
        w_query,
        w_keyval.T,
        positions.reshape(-1, 128),
        jnp.asarray(freq),
        keyval_order,
    )
    return pl.pallas_call(
        pass_on,
        out_shape=outs,
        in_specs=[hbm, hbm],
        out_specs=(hbm, hbm),
        scratch_shapes=[pltpu.VMEM(out.shape, out.dtype) for out in outs] + [dma((2, 2, 2))],
        name="pass_on",
    )(*results)


def solution(mesh):
    in_specs = (
        P(("gx", "gy"), "gz"),
        P("gz"),
        P("gz", ("gx", "gy")),
        P("gz", ("gx", "gy")),
        P("gz"),
        P(),
    )
    out_specs = (P("gz", ("gx", "gy")), P("gy", "gz", None))
    return jax.shard_map(body, mesh=mesh, in_specs=in_specs, out_specs=out_specs, check_vma=False)
```

```python
import functools
import math

import jax
import jax.numpy as jnp
import numpy as np
from jax import lax
from jax.experimental import pallas as pl
from jax.experimental.pallas import tpu as pltpu
from jax.sharding import PartitionSpec as P

D = 16384
KVH = 8
HD = 128
rope_base = 500000.0
norm_eps = 1e-05

MESH = pl.DeviceIdType.MESH
F32 = jnp.float32
BF16 = jnp.bfloat16

O, L, R, F = 0, 3, 1, 2

ARRIVALS = [
    [],
    [(L, O, 0), (R, O, 1)],
    [(L, O, 1), (R, O, 0)],
    [(O, L, 0), (O, R, 1), "weights_own"],
    [(F, O, 0), (F, O, 1)],
    [(L, L, 0), (R, R, 1)],
    [(O, L, 1), (O, R, 0)],
    [(L, R, 1), (R, L, 0)],
    [(L, L, 1), (R, R, 0)],
    [(O, F, 0), (O, F, 1)],
    ["weights_near", (L, R, 0), (R, L, 1)],
    [(F, L, 0), (F, R, 1)],
    [(L, F, 0), (R, F, 1)],
    ["weights_far", "kv_products", (L, F, 1), (R, F, 0)],
    ["kv_relay", (F, R, 0), (F, L, 1)],
    ["kv_plane", (F, F, 0), (F, F, 1)],
]
STEPS = [(O, O, 0), (O, O, 1)] + [e for events in ARRIVALS for e in events if not isinstance(e, str)]
N_STEPS = len(STEPS)
PAIR = {step: n // 2 for n, step in enumerate(STEPS)}

SLOTS = [(events, max(2 * n, 2), max(2 * n - 4, 0), max(2 * n - 8, 0)) for n, events in enumerate(ARRIVALS)] + [
    ([], 32, 26, 22),
    (["kv_owner"], 32, 30, 26),
    (["kv_near"], 32, 32, 28),
    (["kv_far"], 32, 32, 32),
]
KV_STEPS = (O, L, R, F)

KV_EVENTS = [
    [(O, L, 0), (O, R, 1)], [(L, O, 0), (R, O, 1)], [(O, L, 1), (O, R, 0)], [(L, O, 1), (R, O, 0)], [(O, F, 0), (O, F, 1)],
    [(L, L, 0), (R, R, 1)], [(L, R, 0), (R, L, 1)], [(L, F, 0), (R, F, 1)],
    [(F, O, 0), (F, O, 1)], [(L, R, 1), (R, L, 0)], [(L, L, 1), (R, R, 0)], [(F, L, 0), (F, R, 1)],
    [(L, F, 1), (R, F, 0)], [(F, R, 0), (F, L, 1)], [(F, F, 0), (F, F, 1)],
]


def lookup(t, values):
    return sum((t == k).astype(jnp.int32) * v for k, v in enumerate(values) if v)


def fused(
    h_hbm, gain_ref, wq_hbm, wkv_hbm, pos_ref, freq_ref, order_ref,
    q_hbm, kv_hbm,
    rows, wq, w, wkv, w_kv, part, part_kv, inbox, inbox_kv, kvs, factors, cosines, sines,
    load_sem, a_send, a_recv, a_side_send, a_side_recv,
    k_send, k_recv, k_side_send, k_side_recv, r_send, r_recv, r_kv_send, r_kv_recv,
    w_send, w_recv, q_ref, kv_ref, out_sem,
):
    gx, gy, gz = lax.axis_index("gx"), lax.axis_index("gy"), lax.axis_index("gz")
    x, core, zh = gx // 2, gx % 2, gy
    zl, y = gz // 4, gz % 4
    tok = rows.shape[2]
    part_tok = tok // 2
    kdim = rows.shape[3]
    n_q = wq.shape[1]
    n_kv = wkv.shape[1]
    n_head = 4 * n_kv

    def at(xx, cc, zz, yy, ll):
        return (2 * xx + cc, zz, ll * 4 + yy)

    sibling = at(x, 1 - core, zh, y, zl)
    x_up = at((x + 1) % 4, core, zh, y, zl)
    x_down = at((x + 3) % 4, core, zh, y, zl)
    z_up = at(x, core, (zh + 1) % 4, y, zl)
    z_down = at(x, core, (zh + 3) % 4, y, zl)

    loads = [
        pltpu.make_async_copy(h_hbm, rows.at[gx, gy], load_sem.at[0]),
        pltpu.make_async_copy(wq_hbm, wq, load_sem.at[1]),
        pltpu.make_async_copy(wkv_hbm, wkv.at[gy], load_sem.at[2]),
    ]
    for load in loads:
        load.start()

    barrier = pltpu.get_barrier_semaphore()
    peers = [
        sibling, x_up, x_down, z_up, z_down,
        at(x, core, zh, (y + 1) % 4, zl), at(x, core, zh, (y + 3) % 4, zl), at(x, core, zh, y, 1 - zl),
    ]
    for peer in peers:
        pl.semaphore_signal(barrier, inc=1, device_id=peer, device_id_type=MESH)

    class Gather:
        def __init__(self, buf, sends, recv, side_send, side_recv):
            self.buf, self.sends, self.recv = buf, sends, recv
            self.side_send, self.side_recv = side_send, side_recv
            self.size, self.extra = tok // 2, buf.shape[2] - tok

        def piece(self, ox, oz, p, whole=False):
            size = self.size + (self.extra if whole and p else 0)
            return self.buf.at[2 * ((x + ox) % 4) + core, (zh + oz) % 4, pl.ds(p * self.size, size)]

        def push(self, ox, oz, p, to_x, to_z, target):
            along_z = to_x == O
            ref = self.piece(ox, oz, p, whole=along_z)
            pltpu.make_async_remote_copy(
                src_ref=ref, dst_ref=ref, send_sem=self.sends.at[int(along_z)],
                recv_sem=self.recv.at[PAIR[to_x, to_z, p]], device_id=target, device_id_type=MESH,
            ).start()

        def side(self, ox, oz, p):
            ref = self.piece(ox, oz, p)
            n = PAIR[ox, oz, p] if self.side_recv.shape[0] > 1 else 0
            pltpu.make_async_remote_copy(
                src_ref=ref, dst_ref=ref, send_sem=self.side_send, recv_sem=self.side_recv.at[n],
                device_id=sibling, device_id_type=MESH,
            ).start()

        def begin(self):
            for p in (0, 1):
                self.push(O, O, p, O, L, z_up)
                self.push(O, O, 1 - p, O, R, z_down)
                self.push(O, O, p, L, O, x_up)
                self.push(O, O, 1 - p, R, O, x_down)
            for p in (0, 1):
                self.side(O, O, p)

        def arrive(self, *pieces):
            whole = self.buf.at[0, 0] if pieces[0][0] == O else self.buf.at[0, 0, pl.ds(0, tok)]
            received(whole, self.recv.at[PAIR[pieces[0]]])
            if (O, L, 0) in pieces:
                self.push(O, L, 0, O, F, z_up)
            if (O, R, 1) in pieces:
                self.push(O, R, 1, O, F, z_down)
            for ox, oz, p in pieces:
                if ox == O:
                    self.push(O, oz, p, L, oz, x_up)
                if (ox, p) == (L, 0):
                    self.push(L, oz, 0, F, oz, x_up)
            for ox, oz, p in pieces[::-1]:
                if ox == O:
                    self.push(O, oz, p, R, oz, x_down)
                if (ox, p) == (R, 1):
                    self.push(R, oz, 1, F, oz, x_down)
            for piece in pieces:
                self.side(*piece)

        def finish(self):
            left(self.buf.at[pl.ds(0, 8), pl.ds(0, 3), pl.ds(0, self.size)], self.sends.at[0])
            left(self.buf.at[0, pl.ds(0, 3)], self.sends.at[1])
            left(self.buf.at[:, :, pl.ds(0, self.size)], self.side_send)

    def received(ref, sem):
        pltpu.make_async_remote_copy(
            src_ref=ref, dst_ref=ref, send_sem=a_side_send, recv_sem=sem, device_id=sibling, device_id_type=MESH
        ).wait_recv()

    def left(ref, sem):
        pltpu.make_async_remote_copy(
            src_ref=ref, dst_ref=ref, send_sem=sem, recv_sem=a_recv.at[0], device_id=sibling, device_id_type=MESH
        ).wait_send()

    gather = Gather(rows, a_send, a_recv, a_side_send, a_side_recv)
    kv_gather = Gather(kvs, k_send, k_recv, k_side_send, k_side_recv)

    half_kv = n_kv // 2

    def weights_copy(oz, p, to_z, target):
        ref = wkv.at[(zh + oz) % 4, pl.ds(p * half_kv, half_kv)]
        return pltpu.make_async_remote_copy(
            src_ref=ref, dst_ref=ref, send_sem=w_send, recv_sem=w_recv.at[0 if (to_z, p) in ((L, 0), (R, 1)) else 1],
            device_id=target, device_id_type=MESH,
        )

    weights_sent = [
        (O, 0, L, z_up), (O, 1, R, z_down), (O, 1, L, z_up), (O, 0, R, z_down),
        (L, 0, F, z_up), (R, 1, F, z_down),
    ]

    def weights_own():
        for args in weights_sent[:4]:
            weights_copy(*args).start()

    def weights_near():
        received(wkv.at[0], w_recv.at[0])
        for args in weights_sent[4:]:
            weights_copy(*args).start()

    def weights_far():
        received(wkv.at[pl.ds(0, 2)], w_recv.at[1])
        for g in range(4):
            w_kv[g * n_kv : (g + 1) * n_kv, :] = (wkv[g].astype(F32) * gain_ref[...].astype(F32)[None, :]).astype(BF16)

    loads[0].wait()
    loads[2].wait()
    pl.semaphore_wait(barrier, len(peers))
    gather.begin()

    loads[1].wait()
    side_len = 128
    row_id = lax.broadcasted_iota(jnp.int32, (side_len, side_len), 0)
    lane = lax.broadcasted_iota(jnp.int32, (side_len, side_len), 1)

    for i in range(kdim // side_len):
        band = slice(i * side_len, (i + 1) * side_len)
        gain = jnp.broadcast_to(gain_ref[band].astype(F32)[None, :], (side_len, side_len))
        diagonal = jnp.where(row_id == lane, gain, 0.0).astype(BF16)
        w[band, 0:n_q] = jnp.dot(diagonal, wq[band, :], preferred_element_type=F32).astype(BF16)

    def tables(i, carry):
        spread = jnp.broadcast_to(pos_ref[pl.ds(i, 1), :].astype(F32), (side_len, side_len))
        angles = jnp.transpose(spread) * freq_ref[0:1, :]
        band = pl.ds(pl.multiple_of(i * side_len, side_len), side_len)
        cosines[band, :] = jnp.cos(angles)
        s = jnp.sin(angles)
        sines[band, :] = jnp.where(lane % 2 == 0, -s, s)
        return carry

    lax.fori_loop(0, pos_ref.shape[0], tables, 0)

    def unit(t, xx, c):
        y_own = (2 * xx + c) % 4
        zl_own = xx // 2
        step = 1 + 2 * ((t + c) % 2)
        relay, far, direct = (y_own + step) % 4, (y_own + 2) % 4, (y_own + 4 - step) % 4
        return y_own, zl_own, relay, far, direct

    class Reduction:
        def __init__(self, part, inbox, send, recv):
            self.part, self.inbox, self.send, self.recv = part, inbox, send, recv

        def copy(self, t, c, slot, target):
            return pltpu.make_async_remote_copy(
                src_ref=self.own(t, c), dst_ref=self.inbox.at[t, c, slot], send_sem=self.send,
                recv_sem=self.recv.at[t, c], device_id=target, device_id_type=MESH,
            )

        def landed(self, t, c, count):
            received(self.inbox.at[t, c, pl.ds(0, count)], self.recv.at[t, c])

        def total(self, t, c, slots, band, cols):
            value = self.own(t, c)[band, cols].astype(F32)
            for slot in slots:
                value = value + self.inbox[t, c, slot, band, cols].astype(F32)
            return value

        def first(self, t):
            for c in (0, 1):
                y_own, _, relay, far, direct = unit(t, self.place(t)[0], c)

                @pl.when(y == far)
                def _():
                    self.copy(t, c, 0, at(x, core, zh, relay, zl)).start()

                @pl.when(y == direct)
                def _():
                    self.copy(t, c, 0, at(x, core, zh, y_own, zl)).start()

        def relay(self, t):
            for c in (0, 1):
                y_own, _, relay, far, direct = unit(t, self.place(t)[0], c)

                @pl.when(y == relay)
                def _():
                    self.landed(t, c, 1)
                    self.add_up(t, c, [0])
                    self.copy(t, c, 1, at(x, core, zh, y_own, zl)).start()

        def plane(self, t):
            for c in (0, 1):
                y_own, zl_own, relay, far, direct = unit(t, self.place(t)[0], c)

                @pl.when((y == y_own) & (zl != zl_own))
                def _():
                    self.landed(t, c, 2)
                    self.add_up(t, c, [0, 1])
                    self.copy(t, c, 2, at(x, core, zh, y, zl_own)).start()

        def owner(self, t):
            for c in (0, 1):
                xx, zz = self.place(t)
                y_own, zl_own, relay, far, direct = unit(t, xx, c)

                @pl.when((y == y_own) & (zl == zl_own))
                def _():
                    self.landed(t, c, 3)
                    self.store(t, c, zz)

    tile_lane = lax.broadcasted_iota(jnp.int32, (tok, 128), 1)
    short_row = lax.broadcasted_iota(jnp.int32, (16, 128), 0)

    def rotate(tile, cos_t, sin_t):
        swapped = jnp.where(tile_lane[: tile.shape[0]] % 2 == 0, pltpu.roll(tile, 127, 1), pltpu.roll(tile, 1, 1))
        return tile * cos_t + swapped * sin_t

    class QueryReduction(Reduction):
        def place(self, t):
            return (x + lookup(t, [s[0] for s in STEPS])) % 4, (zh + lookup(t, [s[1] for s in STEPS])) % 4

        def own(self, t, c):
            return self.part.at[t, c]

        def rows_of(self, t):
            return lookup(t, [s[2] for s in STEPS]) * part_tok

        def add_up(self, t, c, slots):
            for n0 in range(0, n_q, 128):
                cols = slice(n0, n0 + 128)
                self.own(t, c)[:, cols] = self.total(t, c, slots, slice(None), cols).astype(BF16)

        def store(self, t, c, zz):
            band = pl.ds(pl.multiple_of(zz * tok + self.rows_of(t), part_tok), part_tok)
            cos_t, sin_t, factor = cosines[band, :], sines[band, :], factors[band, :]
            for n0 in range(0, n_q, 128):
                cols = slice(n0, n0 + 128)
                value = self.total(t, c, range(3), slice(None), cols) * factor
                q_ref[band, cols] = rotate(value, cos_t, sin_t).astype(BF16)

    class KeyValueReduction(Reduction):
        def place(self, k):
            return (x + lookup(k, KV_STEPS)) % 4, zh

        def own(self, k, c):
            return self.part.at[2 * k + c]

        def add_up(self, t, c, slots):
            tile = self.total(t, c, slots, pl.ds(tok, 16), slice(0, 128))
            rest = tile - tile.astype(BF16).astype(F32)
            tile = jnp.where(short_row == 1, tile + pltpu.roll(rest, 1, 0), tile)
            self.own(t, c)[tok : tok + 16, 0:128] = tile.astype(BF16)
            for n0 in range(0, n_head, 128):
                cols = slice(n0, n0 + 128)
                self.own(t, c)[0:tok, cols] = self.total(t, c, slots, pl.ds(0, tok), cols).astype(BF16)

        def store(self, t, c, zz):
            band = pl.ds(pl.multiple_of(zz * tok, tok), tok)
            tile = self.total(t, c, range(3), pl.ds(tok, 16), slice(0, 128))
            square = jnp.sum(jnp.where(short_row < 2, tile, 0.0), axis=0, keepdims=True)
            factor = lax.rsqrt(square / D + norm_eps)
            first = factor.astype(BF16).astype(F32)
            second = (factor - first).astype(BF16).astype(F32)
            third = factor - first - second
            spread = jnp.where(short_row == 0, first, jnp.where(short_row == 1, second, third))
            kvs[gx, gy, tok : tok + 16, 0:128] = spread.astype(BF16)
            kvs[gx, gy, tok : tok + 16, 128:256] = jnp.zeros((16, 128), BF16)
            factor = jnp.transpose(jnp.broadcast_to(factor, (tok, 128)))
            everything = pl.ds(0, tok)
            key = self.total(t, c, range(3), everything, slice(0, 128)) * factor
            kvs[gx, gy, 0:tok, 0:128] = rotate(key, cosines[band, :], sines[band, :]).astype(BF16)
            value = self.total(t, c, range(3), everything, slice(128, 256)) * factor
            kvs[gx, gy, 0:tok, 128:256] = value.astype(BF16)

    query = QueryReduction(part, inbox, r_send, r_recv)
    keyval = KeyValueReduction(part_kv, inbox_kv, r_kv_send, r_kv_recv)

    def compute(t):
        xx, zz = query.place(t)
        p = lookup(t, [s[2] for s in STEPS])

        @pl.when(t % 2 == 0)
        def _():
            received(rows.at[0, 0], a_side_recv.at[t // 2])

        band = pl.ds(pl.multiple_of(p * part_tok, part_tok), part_tok)
        lhs = rows[pl.ds(2 * xx, 2), zz, band].reshape(tok, kdim)
        for n0 in range(0, n_q, 256):
            c_tile = jnp.dot(lhs, w[:, n0 : n0 + 256], preferred_element_type=F32).astype(BF16)
            part[t, 0, :, n0 : n0 + 256] = c_tile[:part_tok]
            part[t, 1, :, n0 : n0 + 256] = c_tile[part_tok:]
        query.first(t)

    def spread_factor(oz):
        zz = (zh + oz) % 4
        pieces = kvs[gx, zz, tok : tok + 16, 0:128].astype(F32)
        factor = jnp.sum(jnp.where(short_row < 3, pieces, 0.0), axis=0, keepdims=True)
        band = pl.ds(pl.multiple_of(zz * tok, tok), tok)
        factors[band, :] = jnp.transpose(jnp.broadcast_to(factor, (tok, 128)))

    wide_lane = lax.broadcasted_iota(jnp.int32, (2 * tok, 128), 1)

    def kv_product(k):
        xx, zz = keyval.place(k)
        pair = pl.ds(2 * xx, 2)
        squares = jnp.zeros((2 * tok, 128), F32)
        for k0 in range(0, kdim, 128):
            some = rows[pair, zz, :, k0 : k0 + 128].reshape(2 * tok, 128).astype(F32)
            squares = squares + some * some
        square = jnp.sum(squares, axis=1, keepdims=True)
        high = square.astype(BF16).astype(F32)
        spread = jnp.where(wide_lane == 0, high, jnp.where(wide_lane == 1, square - high, 0.0))
        lhs = rows[pair, zz].reshape(2 * tok, kdim)
        tile = lax.dot_general(lhs, w_kv[...], (((1,), (1,)), ((), ())), preferred_element_type=F32).astype(BF16)
        for c in (0, 1):
            part_kv[2 * k + c, 0:tok, :] = tile[c * tok : (c + 1) * tok]
            turned = jnp.transpose(spread[c * tok : (c + 1) * tok])
            part_kv[2 * k + c, tok : tok + 16, 0:128] = turned[0:16].astype(BF16)
            part_kv[2 * k + c, tok : tok + 16, 128:256] = jnp.zeros((16, 128), BF16)
        keyval.first(k)

    def stages(stage, begin, end=N_STEPS):
        lax.fori_loop(begin, end, lambda t, carry: (stage(t), carry)[1], 0)

    named = {
        "kv_near": lambda: [kv_gather.arrive(*pieces) for pieces in KV_EVENTS[:4]],
        "kv_far": lambda: kv_gather.arrive(*KV_EVENTS[4]),
        "weights_near": weights_near,
        "weights_far": weights_far,
        "kv_products": lambda: stages(kv_product, 0, 4),
        "kv_relay": lambda: stages(keyval.relay, 0, 4),
        "kv_owner": lambda: (stages(keyval.owner, 0, 4), kv_gather.begin()),
        "kv_plane": lambda: stages(keyval.plane, 0, 4),
    }

    def slot(n, carry):
        for k, (events, _, _, _) in enumerate(SLOTS):
            if events:

                @pl.when(n == k)
                def _():
                    for event in events:
                        if isinstance(event, str) and event != "weights_own":
                            named[event]()
                    pieces = [event for event in events if not isinstance(event, str)]
                    if pieces:
                        gather.arrive(*pieces)
                    if "weights_own" in events:
                        weights_own()

        for at_slot, stage in ((1, compute), (2, query.relay), (3, query.plane)):
            counts = [s[at_slot] for s in SLOTS]
            stages(stage, lookup(n, [0] + counts[:-1]), lookup(n, counts))
        return carry

    lax.fori_loop(0, len(SLOTS), slot, 0)

    def owner_near(t):
        @pl.when(lookup(t, [int(s[1] != F) for s in STEPS]) == 1)
        def _():
            query.owner(t)

    def owner_far(t):
        @pl.when(lookup(t, [int(s[1] == F) for s in STEPS[:28]] + [1] * 4) == 1)
        def _():
            query.owner(t)

    kv_gather.arrive(*KV_EVENTS[5])
    for oz in (O, L, R):
        spread_factor(oz)
    stages(owner_near, 0, 16)
    kv_gather.arrive(*KV_EVENTS[6])
    stages(owner_near, 16, 28)
    kv_gather.arrive(*KV_EVENTS[7])
    spread_factor(F)
    stages(owner_far, 0)
    q_out = pltpu.make_async_copy(q_ref, q_hbm, out_sem.at[0])
    q_out.start()
    for event in KV_EVENTS[8:]:
        kv_gather.arrive(*event)
    received(kvs.at[:, :, pl.ds(0, tok // 2)], k_side_recv.at[0])
    slots = kv_ref.shape[0]
    for s in range(slots):
        head = order_ref[slots * gy + s]
        for g in range(4):
            kv_ref[s, g * tok : (g + 1) * tok, :] = kvs[head, g, 0:tok, :]
    kv_out = pltpu.make_async_copy(kv_ref, kv_hbm, out_sem.at[1])
    kv_out.start()

    gather.finish()
    kv_gather.finish()

    left(wkv.at[pl.ds(0, 3)], w_send)
    owned = N_STEPS // 4
    left(part.at[pl.ds(0, N_STEPS - owned // 2)], r_send)
    left(part_kv.at[pl.ds(0, 7)], r_kv_send)
    q_out.wait()
    kv_out.wait()


def pass_on(q_in, kv_in, q_out, kv_out, q_buf, kv_buf, sems):
    takes, puts = [], []
    for n, (source, buf, target) in enumerate(((q_in, q_buf, q_out), (kv_in, kv_buf, kv_out))):
        half = buf.shape[0] // 2
        for i in (0, 1):
            piece = pl.ds(i * half, half)
            takes.append(pltpu.make_async_copy(source.at[piece], buf.at[piece], sems.at[0, n, i]))
            puts.append(pltpu.make_async_copy(buf.at[piece], target.at[piece], sems.at[1, n, i]))
    for take in takes:
        take.start()
    for take, put in zip(takes, puts):
        take.wait()
        put.start()
    for put in puts:
        put.wait()


def body(hidden_rows, norm_gain, w_query, w_keyval, positions, keyval_order):
    tok, kdim = hidden_rows.shape
    n_q, n_kv = w_query.shape[1], w_keyval.shape[1]
    n_head = 4 * n_kv
    n_tok = positions.shape[0]
    freq = np.exp((np.arange(128) // 2) * (-2.0 * math.log(rope_base) / HD)).astype(np.float32)[None, :]
    hbm = pl.BlockSpec(memory_space=pl.ANY)
    vmem = pl.BlockSpec(memory_space=pltpu.VMEM)
    dma = pltpu.SemaphoreType.DMA
    outs = (
        jax.ShapeDtypeStruct((n_tok, n_q), BF16),
        jax.ShapeDtypeStruct((2, n_tok, 2 * HD), BF16),
    )
    results = pl.pallas_call(
        fused,
        out_shape=outs,
        in_specs=[hbm, vmem, hbm, hbm, vmem, vmem, pl.BlockSpec(memory_space=pltpu.SMEM)],
        out_specs=(hbm, hbm),
        scratch_shapes=[
            pltpu.VMEM((8, 4, tok, kdim), BF16),
            pltpu.VMEM((kdim, n_q), BF16),
            pltpu.VMEM((kdim, n_q), BF16),
            pltpu.VMEM((4, n_kv, kdim), BF16),
            pltpu.VMEM((n_head, kdim), BF16),
            pltpu.VMEM((N_STEPS, 2, tok // 2, n_q), BF16),
            pltpu.VMEM((8, tok + 16, n_head), BF16),
            pltpu.VMEM((N_STEPS, 2, 3, tok // 2, n_q), BF16),
            pltpu.VMEM((4, 2, 3, tok + 16, n_head), BF16),
            pltpu.VMEM((8, 4, tok + 16, n_head), BF16),
            pltpu.VMEM((n_tok, 128), F32),
            pltpu.VMEM((n_tok, 128), F32),
            pltpu.VMEM((n_tok, 128), F32),
            dma((3,)),
            dma((2,)), dma((N_STEPS // 2,)), dma(()), dma((N_STEPS // 2,)),
            dma((2,)), dma((N_STEPS // 2,)), dma(()), dma((1,)),
            dma(()), dma((N_STEPS, 2)), dma(()), dma((4, 2)),
            dma(()), dma((2,)),
            pltpu.VMEM((n_tok, n_q), BF16),
            pltpu.VMEM((2, n_tok, 2 * HD), BF16),
            dma((2,)),
        ],
        compiler_params=pltpu.CompilerParams(
            collective_id=0, has_side_effects=True, vmem_limit_bytes=62 * 1024 * 1024
        ),
        name="fused",
    )(
        hidden_rows,
        norm_gain,
        w_query,
        w_keyval.T,
        positions.reshape(-1, 128),
        jnp.asarray(freq),
        keyval_order,
    )
    return pl.pallas_call(
        pass_on,
        out_shape=outs,
        in_specs=[hbm, hbm],
        out_specs=(hbm, hbm),
        scratch_shapes=[pltpu.VMEM(out.shape, out.dtype) for out in outs] + [dma((2, 2, 2))],
        name="pass_on",
    )(*results)


def solution(mesh):
    in_specs = (
        P(("gx", "gy"), "gz"),
        P("gz"),
        P("gz", ("gx", "gy")),
        P("gz", ("gx", "gy")),
        P("gz"),
        P(),
    )
    out_specs = (P("gz", ("gx", "gy")), P("gy", "gz", None))
    return jax.shard_map(body, mesh=mesh, in_specs=in_specs, out_specs=out_specs, check_vma=False)
```

```python
import functools
import math

import jax
import jax.numpy as jnp
import numpy as np
from jax import lax
from jax.experimental import pallas as pl
from jax.experimental.pallas import tpu as pltpu
from jax.sharding import PartitionSpec as P

D = 16384
KVH = 8
HD = 128
rope_base = 500000.0
norm_eps = 1e-05

MESH = pl.DeviceIdType.MESH
F32 = jnp.float32
BF16 = jnp.bfloat16

O, L, R, F = 0, 3, 1, 2

ARRIVALS = [
    [],
    [(L, O, 0), (R, O, 1)],
    [(L, O, 1), (R, O, 0)],
    [(O, L, 0), (O, R, 1), "weights_own"],
    [(F, O, 0), (F, O, 1)],
    [(L, L, 0), (R, R, 1)],
    [(O, L, 1), (O, R, 0)],
    ["weights_near", (L, R, 1), (R, L, 0)],
    [(L, L, 1), (R, R, 0)],
    [(L, R, 0), (R, L, 1)],
    ["weights_far", "kv_products", (F, L, 0), (F, R, 1)],
    [(O, F, 0), (O, F, 1)],
    ["kv_relay", (F, R, 0), (F, L, 1)],
    ["kv_plane", (L, F, 0), (R, F, 1)],
    ["kv_owner", (L, F, 1), (R, F, 0)],
    ["kv_z", (F, F, 0), (F, F, 1)],
]
STEPS = [(O, O, 0), (O, O, 1)] + [e for events in ARRIVALS for e in events if not isinstance(e, str)]
N_STEPS = len(STEPS)
PAIR = {step: n // 2 for n, step in enumerate(STEPS)}

def slot_counts(n):
    lag = 4 if n < 11 else 2
    return max(2 * n, 2), max(2 * n - lag, 0), max(2 * n - 2 * lag, 0)


SLOTS = [(events, *slot_counts(n)) for n, events in enumerate(ARRIVALS[:-1])] + [
    ([], 30, 28, 26),
    (ARRIVALS[-1], 32, 30, 28),
    (["kv_far"], 32, 32, 30),
    (["kv_x", "owner_early"], 32, 32, 32),
]
KV_STEPS = (O, L, R, F)

KV_Z = [[(O, L, 0), (O, R, 1)], [(O, L, 1), (O, R, 0)]]
KV_FAR = [[(O, F, 0), (O, F, 1)], [(L, O, 0), (R, O, 1)]]
KV_X = [[(L, O, 1), (R, O, 0)], [(L, L, 0), (R, R, 1)], [(L, R, 0), (R, L, 1)]]
KV_LAST = [
    [(L, F, 0), (R, F, 1)], [(F, O, 0), (F, O, 1)], [(L, R, 1), (R, L, 0)], [(L, L, 1), (R, R, 0)],
    [(F, L, 0), (F, R, 1)], [(L, F, 1), (R, F, 0)], [(F, R, 0), (F, L, 1)], [(F, F, 0), (F, F, 1)],
]
EARLY = 24


def lookup(t, values):
    return sum((t == k).astype(jnp.int32) * v for k, v in enumerate(values) if v)


def fused(
    h_hbm, gain_ref, wq_hbm, wkv_hbm, pos_ref, freq_ref, order_ref,
    q_hbm, kv_hbm,
    rows, wq, w, wkv, w_kv, part, part_kv, inbox, inbox_kv, kvs, factors, cosines, sines,
    load_sem, a_send, a_recv, a_side_send, a_side_recv,
    k_send, k_recv, k_side_send, k_side_recv, r_send, r_recv, r_kv_send, r_kv_recv,
    w_send, w_recv, q_ref, kv_ref, out_sem,
):
    gx, gy, gz = lax.axis_index("gx"), lax.axis_index("gy"), lax.axis_index("gz")
    x, core, zh = gx // 2, gx % 2, gy
    zl, y = gz // 4, gz % 4
    tok = rows.shape[2]
    part_tok = tok // 2
    kdim = rows.shape[3]
    n_q = wq.shape[1]
    n_kv = wkv.shape[1]
    n_head = 4 * n_kv

    def at(xx, cc, zz, yy, ll):
        return (2 * xx + cc, zz, ll * 4 + yy)

    sibling = at(x, 1 - core, zh, y, zl)
    x_up = at((x + 1) % 4, core, zh, y, zl)
    x_down = at((x + 3) % 4, core, zh, y, zl)
    z_up = at(x, core, (zh + 1) % 4, y, zl)
    z_down = at(x, core, (zh + 3) % 4, y, zl)

    loads = [
        pltpu.make_async_copy(h_hbm, rows.at[gx, gy], load_sem.at[0]),
        pltpu.make_async_copy(wq_hbm, wq, load_sem.at[1]),
        pltpu.make_async_copy(wkv_hbm, wkv.at[gy], load_sem.at[2]),
    ]
    for load in loads:
        load.start()

    barrier = pltpu.get_barrier_semaphore()
    peers = [
        sibling, x_up, x_down, z_up, z_down,
        at(x, core, zh, (y + 1) % 4, zl), at(x, core, zh, (y + 3) % 4, zl), at(x, core, zh, y, 1 - zl),
    ]
    for peer in peers:
        pl.semaphore_signal(barrier, inc=1, device_id=peer, device_id_type=MESH)

    class Gather:
        def __init__(self, buf, sends, recv, side_send, side_recv):
            self.buf, self.sends, self.recv = buf, sends, recv
            self.side_send, self.side_recv = side_send, side_recv
            self.size, self.extra = tok // 2, buf.shape[2] - tok

        def piece(self, ox, oz, p, whole=False):
            size = self.size + (self.extra if whole and p else 0)
            return self.buf.at[2 * ((x + ox) % 4) + core, (zh + oz) % 4, pl.ds(p * self.size, size)]

        def push(self, ox, oz, p, to_x, to_z, target):
            along_z = to_x == O
            ref = self.piece(ox, oz, p, whole=along_z)
            pltpu.make_async_remote_copy(
                src_ref=ref, dst_ref=ref, send_sem=self.sends.at[int(along_z)],
                recv_sem=self.recv.at[PAIR[to_x, to_z, p]], device_id=target, device_id_type=MESH,
            ).start()

        def side(self, ox, oz, p):
            ref = self.piece(ox, oz, p)
            n = PAIR[ox, oz, p] if self.side_recv.shape[0] > 1 else 0
            pltpu.make_async_remote_copy(
                src_ref=ref, dst_ref=ref, send_sem=self.side_send, recv_sem=self.side_recv.at[n],
                device_id=sibling, device_id_type=MESH,
            ).start()

        def begin(self):
            for p in (0, 1):
                self.push(O, O, p, O, L, z_up)
                self.push(O, O, 1 - p, O, R, z_down)
                self.push(O, O, p, L, O, x_up)
                self.push(O, O, 1 - p, R, O, x_down)
            for p in (0, 1):
                self.side(O, O, p)

        def forward_z(self):
            self.push(O, L, 0, O, F, z_up)
            self.push(O, R, 1, O, F, z_down)

        def arrive(self, *pieces, late=False):
            whole = self.buf.at[0, 0] if pieces[0][0] == O else self.buf.at[0, 0, pl.ds(0, tok)]
            received(whole, self.recv.at[PAIR[pieces[0]]])
            if pieces[0] == (O, L, 0) and not late:
                self.forward_z()
            for ox, oz, p in pieces:
                if ox == O:
                    self.push(O, oz, p, L, oz, x_up)
                if (ox, p) == (L, 0):
                    self.push(L, oz, 0, F, oz, x_up)
            for ox, oz, p in pieces[::-1]:
                if ox == O:
                    self.push(O, oz, p, R, oz, x_down)
                if (ox, p) == (R, 1):
                    self.push(R, oz, 1, F, oz, x_down)
            for piece in pieces:
                self.side(*piece)

        def finish(self):
            left(self.buf.at[pl.ds(0, 8), pl.ds(0, 3), pl.ds(0, self.size)], self.sends.at[0])
            left(self.buf.at[0, pl.ds(0, 3)], self.sends.at[1])
            left(self.buf.at[:, :, pl.ds(0, self.size)], self.side_send)

    def received(ref, sem):
        pltpu.make_async_remote_copy(
            src_ref=ref, dst_ref=ref, send_sem=a_side_send, recv_sem=sem, device_id=sibling, device_id_type=MESH
        ).wait_recv()

    def left(ref, sem):
        pltpu.make_async_remote_copy(
            src_ref=ref, dst_ref=ref, send_sem=sem, recv_sem=a_recv.at[0], device_id=sibling, device_id_type=MESH
        ).wait_send()

    gather = Gather(rows, a_send, a_recv, a_side_send, a_side_recv)
    kv_gather = Gather(kvs, k_send, k_recv, k_side_send, k_side_recv)

    half_kv = n_kv // 2

    def weights_copy(oz, p, to_z, target):
        ref = wkv.at[(zh + oz) % 4, pl.ds(p * half_kv, half_kv)]
        return pltpu.make_async_remote_copy(
            src_ref=ref, dst_ref=ref, send_sem=w_send, recv_sem=w_recv.at[0 if (to_z, p) in ((L, 0), (R, 1)) else 1],
            device_id=target, device_id_type=MESH,
        )

    weights_sent = [
        (O, 0, L, z_up), (O, 1, R, z_down), (O, 1, L, z_up), (O, 0, R, z_down),
        (L, 0, F, z_up), (R, 1, F, z_down),
    ]

    def weights_own():
        for args in weights_sent[:4]:
            weights_copy(*args).start()

    def weights_near():
        received(wkv.at[0], w_recv.at[0])
        for args in weights_sent[4:]:
            weights_copy(*args).start()
        gather.forward_z()

    def weights_far():
        received(wkv.at[pl.ds(0, 2)], w_recv.at[1])
        for g in range(4):
            w_kv[g * n_kv : (g + 1) * n_kv, :] = (wkv[g].astype(F32) * gain_ref[...].astype(F32)[None, :]).astype(BF16)

    loads[0].wait()
    loads[2].wait()
    pl.semaphore_wait(barrier, len(peers))
    gather.begin()

    loads[1].wait()
    side_len = 128
    row_id = lax.broadcasted_iota(jnp.int32, (side_len, side_len), 0)
    lane = lax.broadcasted_iota(jnp.int32, (side_len, side_len), 1)

    for i in range(kdim // side_len):
        band = slice(i * side_len, (i + 1) * side_len)
        gain = jnp.broadcast_to(gain_ref[band].astype(F32)[None, :], (side_len, side_len))
        diagonal = jnp.where(row_id == lane, gain, 0.0).astype(BF16)
        w[band, 0:n_q] = jnp.dot(diagonal, wq[band, :], preferred_element_type=F32).astype(BF16)

    def tables(i, carry):
        spread = jnp.broadcast_to(pos_ref[pl.ds(i, 1), :].astype(F32), (side_len, side_len))
        angles = jnp.transpose(spread) * freq_ref[0:1, :]
        band = pl.ds(pl.multiple_of(i * side_len, side_len), side_len)
        cosines[band, :] = jnp.cos(angles)
        s = jnp.sin(angles)
        sines[band, :] = jnp.where(lane % 2 == 0, -s, s)
        return carry

    lax.fori_loop(0, pos_ref.shape[0], tables, 0)

    def unit(t, xx, c):
        y_own = (2 * xx + c) % 4
        zl_own = xx // 2
        step = 1 + 2 * ((t + c) % 2)
        relay, far, direct = (y_own + step) % 4, (y_own + 2) % 4, (y_own + 4 - step) % 4
        return y_own, zl_own, relay, far, direct

    class Reduction:
        def __init__(self, part, inbox, send, recv):
            self.part, self.inbox, self.send, self.recv = part, inbox, send, recv

        def copy(self, t, c, slot, target):
            return pltpu.make_async_remote_copy(
                src_ref=self.own(t, c), dst_ref=self.inbox.at[t, c, slot], send_sem=self.send,
                recv_sem=self.recv.at[t, c], device_id=target, device_id_type=MESH,
            )

        def landed(self, t, c, count):
            received(self.inbox.at[t, c, pl.ds(0, count)], self.recv.at[t, c])

        def total(self, t, c, slots, band, cols):
            value = self.own(t, c)[band, cols].astype(F32)
            for slot in slots:
                value = value + self.inbox[t, c, slot, band, cols].astype(F32)
            return value

        def first(self, t):
            for c in (0, 1):
                y_own, _, relay, far, direct = unit(t, self.place(t)[0], c)

                @pl.when(y == far)
                def _():
                    self.copy(t, c, 0, at(x, core, zh, relay, zl)).start()

                @pl.when(y == direct)
                def _():
                    self.copy(t, c, 0, at(x, core, zh, y_own, zl)).start()

        def relay(self, t):
            for c in (0, 1):
                y_own, _, relay, far, direct = unit(t, self.place(t)[0], c)

                @pl.when(y == relay)
                def _():
                    self.landed(t, c, 1)
                    self.add_up(t, c, [0])
                    self.copy(t, c, 1, at(x, core, zh, y_own, zl)).start()

        def plane(self, t):
            for c in (0, 1):
                y_own, zl_own, relay, far, direct = unit(t, self.place(t)[0], c)

                @pl.when((y == y_own) & (zl != zl_own))
                def _():
                    self.landed(t, c, 2)
                    self.add_up(t, c, [0, 1])
                    self.copy(t, c, 2, at(x, core, zh, y, zl_own)).start()

        def owner(self, t):
            for c in (0, 1):
                xx, zz = self.place(t)
                y_own, zl_own, relay, far, direct = unit(t, xx, c)

                @pl.when((y == y_own) & (zl == zl_own))
                def _():
                    self.landed(t, c, 3)
                    self.store(t, c, zz)

    tile_lane = lax.broadcasted_iota(jnp.int32, (tok, 128), 1)
    short_row = lax.broadcasted_iota(jnp.int32, (16, 128), 0)

    def rotate(tile, cos_t, sin_t):
        swapped = jnp.where(tile_lane[: tile.shape[0]] % 2 == 0, pltpu.roll(tile, 127, 1), pltpu.roll(tile, 1, 1))
        return tile * cos_t + swapped * sin_t

    class QueryReduction(Reduction):
        def place(self, t):
            return (x + lookup(t, [s[0] for s in STEPS])) % 4, (zh + lookup(t, [s[1] for s in STEPS])) % 4

        def own(self, t, c):
            return self.part.at[t, c]

        def rows_of(self, t):
            return lookup(t, [s[2] for s in STEPS]) * part_tok

        def add_up(self, t, c, slots):
            for n0 in range(0, n_q, 128):
                cols = slice(n0, n0 + 128)
                self.own(t, c)[:, cols] = self.total(t, c, slots, slice(None), cols).astype(BF16)

        def store(self, t, c, zz):
            band = pl.ds(pl.multiple_of(zz * tok + self.rows_of(t), part_tok), part_tok)
            cos_t, sin_t, factor = cosines[band, :], sines[band, :], factors[band, :]
            for n0 in range(0, n_q, 128):
                cols = slice(n0, n0 + 128)
                value = self.total(t, c, range(3), slice(None), cols) * factor
                q_ref[band, cols] = rotate(value, cos_t, sin_t).astype(BF16)

    class KeyValueReduction(Reduction):
        def place(self, k):
            return (x + lookup(k, KV_STEPS)) % 4, zh

        def own(self, k, c):
            return self.part.at[2 * k + c]

        def add_up(self, t, c, slots):
            tile = self.total(t, c, slots, pl.ds(tok, 16), slice(0, 128))
            rest = tile - tile.astype(BF16).astype(F32)
            tile = jnp.where(short_row == 1, tile + pltpu.roll(rest, 1, 0), tile)
            self.own(t, c)[tok : tok + 16, 0:128] = tile.astype(BF16)
            for n0 in range(0, n_head, 128):
                cols = slice(n0, n0 + 128)
                self.own(t, c)[0:tok, cols] = self.total(t, c, slots, pl.ds(0, tok), cols).astype(BF16)

        def store(self, t, c, zz):
            band = pl.ds(pl.multiple_of(zz * tok, tok), tok)
            tile = self.total(t, c, range(3), pl.ds(tok, 16), slice(0, 128))
            square = jnp.sum(jnp.where(short_row < 2, tile, 0.0), axis=0, keepdims=True)
            factor = lax.rsqrt(square / D + norm_eps)
            first = factor.astype(BF16).astype(F32)
            second = (factor - first).astype(BF16).astype(F32)
            third = factor - first - second
            spread = jnp.where(short_row == 0, first, jnp.where(short_row == 1, second, third))
            kvs[gx, gy, tok : tok + 16, 0:128] = spread.astype(BF16)
            kvs[gx, gy, tok : tok + 16, 128:256] = jnp.zeros((16, 128), BF16)
            factor = jnp.transpose(jnp.broadcast_to(factor, (tok, 128)))
            everything = pl.ds(0, tok)
            key = self.total(t, c, range(3), everything, slice(0, 128)) * factor
            kvs[gx, gy, 0:tok, 0:128] = rotate(key, cosines[band, :], sines[band, :]).astype(BF16)
            value = self.total(t, c, range(3), everything, slice(128, 256)) * factor
            kvs[gx, gy, 0:tok, 128:256] = value.astype(BF16)

    query = QueryReduction(part, inbox, r_send, r_recv)
    keyval = KeyValueReduction(part_kv, inbox_kv, r_kv_send, r_kv_recv)

    def compute(t):
        xx, zz = query.place(t)
        p = lookup(t, [s[2] for s in STEPS])

        @pl.when(t % 2 == 0)
        def _():
            received(rows.at[0, 0], a_side_recv.at[t // 2])

        band = pl.ds(pl.multiple_of(p * part_tok, part_tok), part_tok)
        lhs = rows[pl.ds(2 * xx, 2), zz, band].reshape(tok, kdim)
        for n0 in range(0, n_q, 256):
            c_tile = jnp.dot(lhs, w[:, n0 : n0 + 256], preferred_element_type=F32).astype(BF16)
            part[t, 0, :, n0 : n0 + 256] = c_tile[:part_tok]
            part[t, 1, :, n0 : n0 + 256] = c_tile[part_tok:]
        query.first(t)

    def spread_factor(oz):
        zz = (zh + oz) % 4
        pieces = kvs[gx, zz, tok : tok + 16, 0:128].astype(F32)
        factor = jnp.sum(jnp.where(short_row < 3, pieces, 0.0), axis=0, keepdims=True)
        band = pl.ds(pl.multiple_of(zz * tok, tok), tok)
        factors[band, :] = jnp.transpose(jnp.broadcast_to(factor, (tok, 128)))

    wide_lane = lax.broadcasted_iota(jnp.int32, (2 * tok, 128), 1)

    def kv_product(k):
        xx, zz = keyval.place(k)
        pair = pl.ds(2 * xx, 2)
        squares = jnp.zeros((2 * tok, 128), F32)
        for k0 in range(0, kdim, 128):
            some = rows[pair, zz, :, k0 : k0 + 128].reshape(2 * tok, 128).astype(F32)
            squares = squares + some * some
        square = jnp.sum(squares, axis=1, keepdims=True)
        high = square.astype(BF16).astype(F32)
        spread = jnp.where(wide_lane == 0, high, jnp.where(wide_lane == 1, square - high, 0.0))
        lhs = rows[pair, zz].reshape(2 * tok, kdim)
        tile = lax.dot_general(lhs, w_kv[...], (((1,), (1,)), ((), ())), preferred_element_type=F32).astype(BF16)
        for c in (0, 1):
            part_kv[2 * k + c, 0:tok, :] = tile[c * tok : (c + 1) * tok]
            turned = jnp.transpose(spread[c * tok : (c + 1) * tok])
            part_kv[2 * k + c, tok : tok + 16, 0:128] = turned[0:16].astype(BF16)
            part_kv[2 * k + c, tok : tok + 16, 128:256] = jnp.zeros((16, 128), BF16)
        keyval.first(k)

    def stages(stage, begin, end=N_STEPS):
        lax.fori_loop(begin, end, lambda t, carry: (stage(t), carry)[1], 0)

    named = {
        "kv_z": lambda: ([kv_gather.arrive(*pieces) for pieces in KV_Z], [spread_factor(oz) for oz in (O, L, R)]),
        "kv_far": lambda: ([kv_gather.arrive(*pieces) for pieces in KV_FAR], spread_factor(F)),
        "kv_x": lambda: [kv_gather.arrive(*pieces) for pieces in KV_X],
        "owner_early": lambda: stages(owner_early, 0, EARLY),
        "weights_near": weights_near,
        "weights_far": weights_far,
        "kv_products": lambda: stages(kv_product, 0, 4),
        "kv_relay": lambda: stages(keyval.relay, 0, 4),
        "kv_owner": lambda: (stages(keyval.owner, 0, 4), kv_gather.begin()),
        "kv_plane": lambda: stages(keyval.plane, 0, 4),
    }

    is_late = [int(s[1] == F) for s in STEPS[:EARLY]] + [1] * (N_STEPS - EARLY)

    def owner_early(t):
        @pl.when(lookup(t, is_late) == 0)
        def _():
            query.owner(t)

    def owner_late(t):
        @pl.when(lookup(t, is_late) == 1)
        def _():
            query.owner(t)

    def slot(n, carry):
        for k, (events, _, _, _) in enumerate(SLOTS):
            if events:

                @pl.when(n == k)
                def _():
                    for event in events:
                        if isinstance(event, str) and event != "weights_own":
                            named[event]()
                    pieces = [event for event in events if not isinstance(event, str)]
                    if pieces:
                        gather.arrive(*pieces, late=True)
                    if "weights_own" in events:
                        weights_own()

        for at_slot, stage in ((1, compute), (2, query.relay), (3, query.plane)):
            counts = [s[at_slot] for s in SLOTS]
            stages(stage, lookup(n, [0] + counts[:-1]), lookup(n, counts))
        return carry

    lax.fori_loop(0, len(SLOTS), slot, 0)

    def owner_near(t):
        @pl.when(lookup(t, [int(s[1] != F) for s in STEPS]) == 1)
        def _():
            query.owner(t)

    def owner_far(t):
        @pl.when(lookup(t, [int(s[1] == F) for s in STEPS[:28]] + [1] * 4) == 1)
        def _():
            query.owner(t)

    kv_gather.arrive(*KV_LAST[0])
    stages(owner_late, 0)
    q_out = pltpu.make_async_copy(q_ref, q_hbm, out_sem.at[0])
    q_out.start()
    for event in KV_LAST[1:]:
        kv_gather.arrive(*event)
    received(kvs.at[:, :, pl.ds(0, tok // 2)], k_side_recv.at[0])
    slots = kv_ref.shape[0]
    for s in range(slots):
        head = order_ref[slots * gy + s]
        for g in range(4):
            kv_ref[s, g * tok : (g + 1) * tok, :] = kvs[head, g, 0:tok, :]
    kv_out = pltpu.make_async_copy(kv_ref, kv_hbm, out_sem.at[1])
    kv_out.start()

    gather.finish()
    kv_gather.finish()

    left(wkv.at[pl.ds(0, 3)], w_send)
    owned = N_STEPS // 4
    left(part.at[pl.ds(0, N_STEPS - owned // 2)], r_send)
    left(part_kv.at[pl.ds(0, 7)], r_kv_send)
    q_out.wait()
    kv_out.wait()


def pass_on(q_in, kv_in, q_out, kv_out, q_buf, kv_buf, sems):
    takes, puts = [], []
    for n, (source, buf, target) in enumerate(((q_in, q_buf, q_out), (kv_in, kv_buf, kv_out))):
        half = buf.shape[0] // 2
        for i in (0, 1):
            piece = pl.ds(i * half, half)
            takes.append(pltpu.make_async_copy(source.at[piece], buf.at[piece], sems.at[0, n, i]))
            puts.append(pltpu.make_async_copy(buf.at[piece], target.at[piece], sems.at[1, n, i]))
    for take in takes:
        take.start()
    for take, put in zip(takes, puts):
        take.wait()
        put.start()
    for put in puts:
        put.wait()


def body(hidden_rows, norm_gain, w_query, w_keyval, positions, keyval_order):
    tok, kdim = hidden_rows.shape
    n_q, n_kv = w_query.shape[1], w_keyval.shape[1]
    n_head = 4 * n_kv
    n_tok = positions.shape[0]
    freq = np.exp((np.arange(128) // 2) * (-2.0 * math.log(rope_base) / HD)).astype(np.float32)[None, :]
    hbm = pl.BlockSpec(memory_space=pl.ANY)
    vmem = pl.BlockSpec(memory_space=pltpu.VMEM)
    dma = pltpu.SemaphoreType.DMA
    outs = (
        jax.ShapeDtypeStruct((n_tok, n_q), BF16),
        jax.ShapeDtypeStruct((2, n_tok, 2 * HD), BF16),
    )
    results = pl.pallas_call(
        fused,
        out_shape=outs,
        in_specs=[hbm, vmem, hbm, hbm, vmem, vmem, pl.BlockSpec(memory_space=pltpu.SMEM)],
        out_specs=(hbm, hbm),
        scratch_shapes=[
            pltpu.VMEM((8, 4, tok, kdim), BF16),
            pltpu.VMEM((kdim, n_q), BF16),
            pltpu.VMEM((kdim, n_q), BF16),
            pltpu.VMEM((4, n_kv, kdim), BF16),
            pltpu.VMEM((n_head, kdim), BF16),
            pltpu.VMEM((N_STEPS, 2, tok // 2, n_q), BF16),
            pltpu.VMEM((8, tok + 16, n_head), BF16),
            pltpu.VMEM((N_STEPS, 2, 3, tok // 2, n_q), BF16),
            pltpu.VMEM((4, 2, 3, tok + 16, n_head), BF16),
            pltpu.VMEM((8, 4, tok + 16, n_head), BF16),
            pltpu.VMEM((n_tok, 128), F32),
            pltpu.VMEM((n_tok, 128), F32),
            pltpu.VMEM((n_tok, 128), F32),
            dma((3,)),
            dma((2,)), dma((N_STEPS // 2,)), dma(()), dma((N_STEPS // 2,)),
            dma((2,)), dma((N_STEPS // 2,)), dma(()), dma((1,)),
            dma(()), dma((N_STEPS, 2)), dma(()), dma((4, 2)),
            dma(()), dma((2,)),
            pltpu.VMEM((n_tok, n_q), BF16),
            pltpu.VMEM((2, n_tok, 2 * HD), BF16),
            dma((2,)),
        ],
        compiler_params=pltpu.CompilerParams(
            collective_id=0, has_side_effects=True, vmem_limit_bytes=62 * 1024 * 1024
        ),
        name="fused",
    )(
        hidden_rows,
        norm_gain,
        w_query,
        w_keyval.T,
        positions.reshape(-1, 128),
        jnp.asarray(freq),
        keyval_order,
    )
    return pl.pallas_call(
        pass_on,
        out_shape=outs,
        in_specs=[hbm, hbm],
        out_specs=(hbm, hbm),
        scratch_shapes=[pltpu.VMEM(out.shape, out.dtype) for out in outs] + [dma((2, 2, 2))],
        name="pass_on",
    )(*results)


def solution(mesh):
    in_specs = (
        P(("gx", "gy"), "gz"),
        P("gz"),
        P("gz", ("gx", "gy")),
        P("gz", ("gx", "gy")),
        P("gz"),
        P(),
    )
    out_specs = (P("gz", ("gx", "gy")), P("gy", "gz", None))
    return jax.shard_map(body, mesh=mesh, in_specs=in_specs, out_specs=out_specs, check_vma=False)
```

```python
import functools
import math

import jax
import jax.numpy as jnp
import numpy as np
from jax import lax
from jax.experimental import pallas as pl
from jax.experimental.pallas import tpu as pltpu
from jax.sharding import PartitionSpec as P

D = 16384
KVH = 8
HD = 128
rope_base = 500000.0
norm_eps = 1e-05

MESH = pl.DeviceIdType.MESH
F32 = jnp.float32
BF16 = jnp.bfloat16

O, L, R, F = 0, 3, 1, 2

ARRIVALS = [
    [],
    [(L, O, 0), (R, O, 1)],
    [(L, O, 1), (R, O, 0)],
    [(O, L, 0), (O, R, 1), "weights_own"],
    [(F, O, 0), (F, O, 1)],
    [(L, L, 0), (R, R, 1)],
    [(O, L, 1), (O, R, 0)],
    ["weights_near", (L, R, 1), (R, L, 0)],
    [(L, L, 1), (R, R, 0)],
    [(L, R, 0), (R, L, 1)],
    ["weights_far", "kv_products", (F, L, 0), (F, R, 1)],
    [(O, F, 0), (O, F, 1)],
    ["kv_relay", (F, R, 0), (F, L, 1)],
    ["kv_plane", (L, F, 0), (R, F, 1)],
    ["kv_owner", (L, F, 1), (R, F, 0)],
    [(F, F, 0), (F, F, 1)],
]
STEPS = [(O, O, 0), (O, O, 1)] + [e for events in ARRIVALS for e in events if not isinstance(e, str)]
N_STEPS = len(STEPS)
PAIR = {step: n // 2 for n, step in enumerate(STEPS)}

def slot_counts(n):
    lag = 4 if n < 13 else 2
    return max(2 * n, 2), max(2 * n - lag, 0), max(2 * n - 2 * lag, 0)


SLOTS = [(events, *slot_counts(n)) for n, events in enumerate(ARRIVALS[:-1])] + [
    ([], 30, 26, 24),
    (ARRIVALS[-1], 30, 28, 26),
    (["kv_z"], 32, 30, 28),
    (["kv_far"], 32, 32, 30),
    (["kv_x", "owner_early"], 32, 32, 32),
]
KV_STEPS = (O, L, R, F)

KV_Z = [[(O, L, 0), (O, R, 1)], [(O, L, 1), (O, R, 0)]]
KV_FAR = [[(O, F, 0), (O, F, 1)], [(L, O, 0), (R, O, 1)]]
KV_X = [[(L, O, 1), (R, O, 0)], [(L, L, 0), (R, R, 1)], [(L, R, 0), (R, L, 1)]]
KV_LAST = [
    [(L, F, 0), (R, F, 1)], [(F, O, 0), (F, O, 1)], [(L, R, 1), (R, L, 0)], [(L, L, 1), (R, R, 0)],
    [(F, L, 0), (F, R, 1)], [(L, F, 1), (R, F, 0)], [(F, R, 0), (F, L, 1)], [(F, F, 0), (F, F, 1)],
]
EARLY = 24


def lookup(t, values):
    return sum((t == k).astype(jnp.int32) * v for k, v in enumerate(values) if v)


def fused(
    h_hbm, gain_ref, wq_hbm, wkv_hbm, pos_ref, freq_ref, order_ref,
    q_hbm, kv_hbm,
    rows, wq, w, wkv, w_kv, part, part_kv, inbox, inbox_kv, kvs, factors, cosines, sines,
    load_sem, a_send, a_recv, a_side_send, a_side_recv,
    k_send, k_recv, k_side_send, k_side_recv, r_send, r_recv, r_kv_send, r_kv_recv,
    w_send, w_recv, q_ref, kv_ref, out_sem,
):
    gx, gy, gz = lax.axis_index("gx"), lax.axis_index("gy"), lax.axis_index("gz")
    x, core, zh = gx // 2, gx % 2, gy
    zl, y = gz // 4, gz % 4
    tok = rows.shape[2]
    part_tok = tok // 2
    kdim = rows.shape[3]
    n_q = wq.shape[1]
    n_kv = wkv.shape[1]
    n_head = 4 * n_kv

    def at(xx, cc, zz, yy, ll):
        return (2 * xx + cc, zz, ll * 4 + yy)

    sibling = at(x, 1 - core, zh, y, zl)
    x_up = at((x + 1) % 4, core, zh, y, zl)
    x_down = at((x + 3) % 4, core, zh, y, zl)
    z_up = at(x, core, (zh + 1) % 4, y, zl)
    z_down = at(x, core, (zh + 3) % 4, y, zl)

    loads = [
        pltpu.make_async_copy(h_hbm, rows.at[gx, gy], load_sem.at[0]),
        pltpu.make_async_copy(wq_hbm, wq, load_sem.at[1]),
        pltpu.make_async_copy(wkv_hbm, wkv.at[gy], load_sem.at[2]),
    ]
    loads[0].start()

    barrier = pltpu.get_barrier_semaphore()
    peers = [
        sibling, x_up, x_down, z_up, z_down,
        at(x, core, zh, (y + 1) % 4, zl), at(x, core, zh, (y + 3) % 4, zl), at(x, core, zh, y, 1 - zl),
    ]
    for peer in peers:
        pl.semaphore_signal(barrier, inc=1, device_id=peer, device_id_type=MESH)

    class Gather:
        def __init__(self, buf, sends, recv, side_send, side_recv):
            self.buf, self.sends, self.recv = buf, sends, recv
            self.side_send, self.side_recv = side_send, side_recv
            self.size, self.extra = tok // 2, buf.shape[2] - tok

        def piece(self, ox, oz, p, whole=False):
            size = self.size + (self.extra if whole and p else 0)
            return self.buf.at[2 * ((x + ox) % 4) + core, (zh + oz) % 4, pl.ds(p * self.size, size)]

        def push(self, ox, oz, p, to_x, to_z, target):
            along_z = to_x == O
            ref = self.piece(ox, oz, p, whole=along_z)
            pltpu.make_async_remote_copy(
                src_ref=ref, dst_ref=ref, send_sem=self.sends.at[int(along_z)],
                recv_sem=self.recv.at[PAIR[to_x, to_z, p]], device_id=target, device_id_type=MESH,
            ).start()

        def side(self, ox, oz, p):
            ref = self.piece(ox, oz, p)
            n = PAIR[ox, oz, p] if self.side_recv.shape[0] > 1 else 0
            pltpu.make_async_remote_copy(
                src_ref=ref, dst_ref=ref, send_sem=self.side_send, recv_sem=self.side_recv.at[n],
                device_id=sibling, device_id_type=MESH,
            ).start()

        def begin(self):
            for p in (0, 1):
                self.push(O, O, p, O, L, z_up)
                self.push(O, O, 1 - p, O, R, z_down)
                self.push(O, O, p, L, O, x_up)
                self.push(O, O, 1 - p, R, O, x_down)
            for p in (0, 1):
                self.side(O, O, p)

        def forward_z(self):
            self.push(O, L, 0, O, F, z_up)
            self.push(O, R, 1, O, F, z_down)

        def arrive(self, *pieces, late=False):
            whole = self.buf.at[0, 0] if pieces[0][0] == O else self.buf.at[0, 0, pl.ds(0, tok)]
            received(whole, self.recv.at[PAIR[pieces[0]]])
            if pieces[0] == (O, L, 0) and not late:
                self.forward_z()
            for ox, oz, p in pieces:
                if ox == O:
                    self.push(O, oz, p, L, oz, x_up)
                if (ox, p) == (L, 0):
                    self.push(L, oz, 0, F, oz, x_up)
            for ox, oz, p in pieces[::-1]:
                if ox == O:
                    self.push(O, oz, p, R, oz, x_down)
                if (ox, p) == (R, 1):
                    self.push(R, oz, 1, F, oz, x_down)
            for piece in pieces:
                self.side(*piece)

        def finish(self):
            left(self.buf.at[pl.ds(0, 8), pl.ds(0, 3), pl.ds(0, self.size)], self.sends.at[0])
            left(self.buf.at[0, pl.ds(0, 3)], self.sends.at[1])
            left(self.buf.at[:, :, pl.ds(0, self.size)], self.side_send)

    def received(ref, sem):
        pltpu.make_async_remote_copy(
            src_ref=ref, dst_ref=ref, send_sem=a_side_send, recv_sem=sem, device_id=sibling, device_id_type=MESH
        ).wait_recv()

    def left(ref, sem):
        pltpu.make_async_remote_copy(
            src_ref=ref, dst_ref=ref, send_sem=sem, recv_sem=a_recv.at[0], device_id=sibling, device_id_type=MESH
        ).wait_send()

    gather = Gather(rows, a_send, a_recv, a_side_send, a_side_recv)
    kv_gather = Gather(kvs, k_send, k_recv, k_side_send, k_side_recv)

    half_kv = n_kv // 2

    def weights_copy(oz, p, to_z, target):
        ref = wkv.at[(zh + oz) % 4, pl.ds(p * half_kv, half_kv)]
        return pltpu.make_async_remote_copy(
            src_ref=ref, dst_ref=ref, send_sem=w_send, recv_sem=w_recv.at[0 if (to_z, p) in ((L, 0), (R, 1)) else 1],
            device_id=target, device_id_type=MESH,
        )

    weights_sent = [
        (O, 0, L, z_up), (O, 1, R, z_down), (O, 1, L, z_up), (O, 0, R, z_down),
        (L, 0, F, z_up), (R, 1, F, z_down),
    ]

    def weights_own():
        for args in weights_sent[:4]:
            weights_copy(*args).start()

    def weights_near():
        received(wkv.at[0], w_recv.at[0])
        for args in weights_sent[4:]:
            weights_copy(*args).start()
        gather.forward_z()

    def weights_far():
        received(wkv.at[pl.ds(0, 2)], w_recv.at[1])
        for g in range(4):
            w_kv[g * n_kv : (g + 1) * n_kv, :] = (wkv[g].astype(F32) * gain_ref[...].astype(F32)[None, :]).astype(BF16)

    loads[0].wait()
    loads[1].start()
    loads[2].start()
    pl.semaphore_wait(barrier, len(peers))
    gather.begin()

    loads[1].wait()
    loads[2].wait()
    side_len = 128
    row_id = lax.broadcasted_iota(jnp.int32, (side_len, side_len), 0)
    lane = lax.broadcasted_iota(jnp.int32, (side_len, side_len), 1)

    for i in range(kdim // side_len):
        band = slice(i * side_len, (i + 1) * side_len)
        gain = jnp.broadcast_to(gain_ref[band].astype(F32)[None, :], (side_len, side_len))
        diagonal = jnp.where(row_id == lane, gain, 0.0).astype(BF16)
        w[band, 0:n_q] = jnp.dot(diagonal, wq[band, :], preferred_element_type=F32).astype(BF16)

    def tables(i, carry):
        spread = jnp.broadcast_to(pos_ref[pl.ds(i, 1), :].astype(F32), (side_len, side_len))
        angles = jnp.transpose(spread) * freq_ref[0:1, :]
        band = pl.ds(pl.multiple_of(i * side_len, side_len), side_len)
        cosines[band, :] = jnp.cos(angles)
        s = jnp.sin(angles)
        sines[band, :] = jnp.where(lane % 2 == 0, -s, s)
        return carry

    lax.fori_loop(0, pos_ref.shape[0], tables, 0)

    def unit(t, xx, c):
        y_own = (2 * xx + c) % 4
        zl_own = xx // 2
        step = 1 + 2 * ((t + c) % 2)
        relay, far, direct = (y_own + step) % 4, (y_own + 2) % 4, (y_own + 4 - step) % 4
        return y_own, zl_own, relay, far, direct

    class Reduction:
        def __init__(self, part, inbox, send, recv):
            self.part, self.inbox, self.send, self.recv = part, inbox, send, recv

        def copy(self, t, c, slot, target):
            return pltpu.make_async_remote_copy(
                src_ref=self.own(t, c), dst_ref=self.inbox.at[t, c, slot], send_sem=self.send,
                recv_sem=self.recv.at[t, c], device_id=target, device_id_type=MESH,
            )

        def landed(self, t, c, count):
            received(self.inbox.at[t, c, pl.ds(0, count)], self.recv.at[t, c])

        def total(self, t, c, slots, band, cols):
            value = self.own(t, c)[band, cols].astype(F32)
            for slot in slots:
                value = value + self.inbox[t, c, slot, band, cols].astype(F32)
            return value

        def first(self, t):
            for c in (0, 1):
                y_own, _, relay, far, direct = unit(t, self.place(t)[0], c)

                @pl.when(y == far)
                def _():
                    self.copy(t, c, 0, at(x, core, zh, relay, zl)).start()

                @pl.when(y == direct)
                def _():
                    self.copy(t, c, 0, at(x, core, zh, y_own, zl)).start()

        def relay(self, t):
            for c in (0, 1):
                y_own, _, relay, far, direct = unit(t, self.place(t)[0], c)

                @pl.when(y == relay)
                def _():
                    self.landed(t, c, 1)
                    self.add_up(t, c, [0])
                    self.copy(t, c, 1, at(x, core, zh, y_own, zl)).start()

        def plane(self, t):
            for c in (0, 1):
                y_own, zl_own, relay, far, direct = unit(t, self.place(t)[0], c)

                @pl.when((y == y_own) & (zl != zl_own))
                def _():
                    self.landed(t, c, 2)
                    self.add_up(t, c, [0, 1])
                    self.copy(t, c, 2, at(x, core, zh, y, zl_own)).start()

        def owner(self, t):
            for c in (0, 1):
                xx, zz = self.place(t)
                y_own, zl_own, relay, far, direct = unit(t, xx, c)

                @pl.when((y == y_own) & (zl == zl_own))
                def _():
                    self.landed(t, c, 3)
                    self.store(t, c, zz)

    tile_lane = lax.broadcasted_iota(jnp.int32, (tok, 128), 1)
    short_row = lax.broadcasted_iota(jnp.int32, (16, 128), 0)

    def rotate(tile, cos_t, sin_t):
        swapped = jnp.where(tile_lane[: tile.shape[0]] % 2 == 0, pltpu.roll(tile, 127, 1), pltpu.roll(tile, 1, 1))
        return tile * cos_t + swapped * sin_t

    class QueryReduction(Reduction):
        def place(self, t):
            return (x + lookup(t, [s[0] for s in STEPS])) % 4, (zh + lookup(t, [s[1] for s in STEPS])) % 4

        def own(self, t, c):
            return self.part.at[t, c]

        def rows_of(self, t):
            return lookup(t, [s[2] for s in STEPS]) * part_tok

        def add_up(self, t, c, slots):
            for n0 in range(0, n_q, 128):
                cols = slice(n0, n0 + 128)
                self.own(t, c)[:, cols] = self.total(t, c, slots, slice(None), cols).astype(BF16)

        def store(self, t, c, zz):
            band = pl.ds(pl.multiple_of(zz * tok + self.rows_of(t), part_tok), part_tok)
            cos_t, sin_t, factor = cosines[band, :], sines[band, :], factors[band, :]
            for n0 in range(0, n_q, 128):
                cols = slice(n0, n0 + 128)
                value = self.total(t, c, range(3), slice(None), cols) * factor
                q_ref[band, cols] = rotate(value, cos_t, sin_t).astype(BF16)

    class KeyValueReduction(Reduction):
        def place(self, k):
            return (x + lookup(k, KV_STEPS)) % 4, zh

        def own(self, k, c):
            return self.part.at[2 * k + c]

        def add_up(self, t, c, slots):
            tile = self.total(t, c, slots, pl.ds(tok, 16), slice(0, 128))
            rest = tile - tile.astype(BF16).astype(F32)
            tile = jnp.where(short_row == 1, tile + pltpu.roll(rest, 1, 0), tile)
            self.own(t, c)[tok : tok + 16, 0:128] = tile.astype(BF16)
            for n0 in range(0, n_head, 128):
                cols = slice(n0, n0 + 128)
                self.own(t, c)[0:tok, cols] = self.total(t, c, slots, pl.ds(0, tok), cols).astype(BF16)

        def store(self, t, c, zz):
            band = pl.ds(pl.multiple_of(zz * tok, tok), tok)
            tile = self.total(t, c, range(3), pl.ds(tok, 16), slice(0, 128))
            square = jnp.sum(jnp.where(short_row < 2, tile, 0.0), axis=0, keepdims=True)
            factor = lax.rsqrt(square / D + norm_eps)
            first = factor.astype(BF16).astype(F32)
            second = (factor - first).astype(BF16).astype(F32)
            third = factor - first - second
            spread = jnp.where(short_row == 0, first, jnp.where(short_row == 1, second, third))
            kvs[gx, gy, tok : tok + 16, 0:128] = spread.astype(BF16)
            kvs[gx, gy, tok : tok + 16, 128:256] = jnp.zeros((16, 128), BF16)
            factor = jnp.transpose(jnp.broadcast_to(factor, (tok, 128)))
            everything = pl.ds(0, tok)
            key = self.total(t, c, range(3), everything, slice(0, 128)) * factor
            kvs[gx, gy, 0:tok, 0:128] = rotate(key, cosines[band, :], sines[band, :]).astype(BF16)
            value = self.total(t, c, range(3), everything, slice(128, 256)) * factor
            kvs[gx, gy, 0:tok, 128:256] = value.astype(BF16)

    query = QueryReduction(part, inbox, r_send, r_recv)
    keyval = KeyValueReduction(part_kv, inbox_kv, r_kv_send, r_kv_recv)

    def compute(t):
        xx, zz = query.place(t)
        p = lookup(t, [s[2] for s in STEPS])

        @pl.when(t % 2 == 0)
        def _():
            received(rows.at[0, 0], a_side_recv.at[t // 2])

        band = pl.ds(pl.multiple_of(p * part_tok, part_tok), part_tok)
        lhs = rows[pl.ds(2 * xx, 2), zz, band].reshape(tok, kdim)
        for n0 in range(0, n_q, 256):
            c_tile = jnp.dot(lhs, w[:, n0 : n0 + 256], preferred_element_type=F32).astype(BF16)
            part[t, 0, :, n0 : n0 + 256] = c_tile[:part_tok]
            part[t, 1, :, n0 : n0 + 256] = c_tile[part_tok:]
        query.first(t)

    def spread_factor(oz):
        zz = (zh + oz) % 4
        pieces = kvs[gx, zz, tok : tok + 16, 0:128].astype(F32)
        factor = jnp.sum(jnp.where(short_row < 3, pieces, 0.0), axis=0, keepdims=True)
        band = pl.ds(pl.multiple_of(zz * tok, tok), tok)
        factors[band, :] = jnp.transpose(jnp.broadcast_to(factor, (tok, 128)))

    wide_lane = lax.broadcasted_iota(jnp.int32, (2 * tok, 128), 1)

    def kv_product(k):
        xx, zz = keyval.place(k)
        pair = pl.ds(2 * xx, 2)
        squares = jnp.zeros((2 * tok, 128), F32)
        for k0 in range(0, kdim, 128):
            some = rows[pair, zz, :, k0 : k0 + 128].reshape(2 * tok, 128).astype(F32)
            squares = squares + some * some
        square = jnp.sum(squares, axis=1, keepdims=True)
        high = square.astype(BF16).astype(F32)
        spread = jnp.where(wide_lane == 0, high, jnp.where(wide_lane == 1, square - high, 0.0))
        lhs = rows[pair, zz].reshape(2 * tok, kdim)
        tile = lax.dot_general(lhs, w_kv[...], (((1,), (1,)), ((), ())), preferred_element_type=F32).astype(BF16)
        for c in (0, 1):
            part_kv[2 * k + c, 0:tok, :] = tile[c * tok : (c + 1) * tok]
            turned = jnp.transpose(spread[c * tok : (c + 1) * tok])
            part_kv[2 * k + c, tok : tok + 16, 0:128] = turned[0:16].astype(BF16)
            part_kv[2 * k + c, tok : tok + 16, 128:256] = jnp.zeros((16, 128), BF16)
        keyval.first(k)

    def stages(stage, begin, end=N_STEPS):
        lax.fori_loop(begin, end, lambda t, carry: (stage(t), carry)[1], 0)

    named = {
        "kv_z": lambda: ([kv_gather.arrive(*pieces) for pieces in KV_Z], [spread_factor(oz) for oz in (O, L, R)]),
        "kv_far": lambda: ([kv_gather.arrive(*pieces) for pieces in KV_FAR], spread_factor(F)),
        "kv_x": lambda: [kv_gather.arrive(*pieces) for pieces in KV_X],
        "owner_early": lambda: stages(owner_early, 0, EARLY),
        "weights_near": weights_near,
        "weights_far": weights_far,
        "kv_products": lambda: stages(kv_product, 0, 4),
        "kv_relay": lambda: stages(keyval.relay, 0, 4),
        "kv_owner": lambda: (stages(keyval.owner, 0, 4), kv_gather.begin()),
        "kv_plane": lambda: stages(keyval.plane, 0, 4),
    }

    is_late = [int(s[1] == F) for s in STEPS[:EARLY]] + [1] * (N_STEPS - EARLY)

    def owner_early(t):
        @pl.when(lookup(t, is_late) == 0)
        def _():
            query.owner(t)

    def owner_late(t):
        @pl.when(lookup(t, is_late) == 1)
        def _():
            query.owner(t)

    def slot(n, carry):
        for k, (events, _, _, _) in enumerate(SLOTS):
            if events:

                @pl.when(n == k)
                def _():
                    for event in events:
                        if isinstance(event, str) and event != "weights_own":
                            named[event]()
                    pieces = [event for event in events if not isinstance(event, str)]
                    if pieces:
                        gather.arrive(*pieces, late=True)
                    if "weights_own" in events:
                        weights_own()

        for at_slot, stage in ((1, compute), (2, query.relay), (3, query.plane)):
            counts = [s[at_slot] for s in SLOTS]
            stages(stage, lookup(n, [0] + counts[:-1]), lookup(n, counts))
        return carry

    lax.fori_loop(0, len(SLOTS), slot, 0)

    def owner_near(t):
        @pl.when(lookup(t, [int(s[1] != F) for s in STEPS]) == 1)
        def _():
            query.owner(t)

    def owner_far(t):
        @pl.when(lookup(t, [int(s[1] == F) for s in STEPS[:28]] + [1] * 4) == 1)
        def _():
            query.owner(t)

    kv_gather.arrive(*KV_LAST[0])
    stages(owner_late, 0)
    q_out = pltpu.make_async_copy(q_ref, q_hbm, out_sem.at[0])
    q_out.start()
    for event in KV_LAST[1:]:
        kv_gather.arrive(*event)
    received(kvs.at[:, :, pl.ds(0, tok // 2)], k_side_recv.at[0])
    slots = kv_ref.shape[0]
    for s in range(slots):
        head = order_ref[slots * gy + s]
        for g in range(4):
            kv_ref[s, g * tok : (g + 1) * tok, :] = kvs[head, g, 0:tok, :]
    kv_out = pltpu.make_async_copy(kv_ref, kv_hbm, out_sem.at[1])
    kv_out.start()

    gather.finish()
    kv_gather.finish()

    left(wkv.at[pl.ds(0, 3)], w_send)
    owned = N_STEPS // 4
    left(part.at[pl.ds(0, N_STEPS - owned // 2)], r_send)
    left(part_kv.at[pl.ds(0, 7)], r_kv_send)
    q_out.wait()
    kv_out.wait()


def pass_on(q_in, kv_in, q_out, kv_out, q_buf, kv_buf, sems):
    takes, puts = [], []
    for n, (source, buf, target) in enumerate(((q_in, q_buf, q_out), (kv_in, kv_buf, kv_out))):
        half = buf.shape[0] // 2
        for i in (0, 1):
            piece = pl.ds(i * half, half)
            takes.append(pltpu.make_async_copy(source.at[piece], buf.at[piece], sems.at[0, n, i]))
            puts.append(pltpu.make_async_copy(buf.at[piece], target.at[piece], sems.at[1, n, i]))
    for take in takes:
        take.start()
    for take, put in zip(takes, puts):
        take.wait()
        put.start()
    for put in puts:
        put.wait()


def body(hidden_rows, norm_gain, w_query, w_keyval, positions, keyval_order):
    tok, kdim = hidden_rows.shape
    n_q, n_kv = w_query.shape[1], w_keyval.shape[1]
    n_head = 4 * n_kv
    n_tok = positions.shape[0]
    freq = np.exp((np.arange(128) // 2) * (-2.0 * math.log(rope_base) / HD)).astype(np.float32)[None, :]
    hbm = pl.BlockSpec(memory_space=pl.ANY)
    vmem = pl.BlockSpec(memory_space=pltpu.VMEM)
    dma = pltpu.SemaphoreType.DMA
    outs = (
        jax.ShapeDtypeStruct((n_tok, n_q), BF16),
        jax.ShapeDtypeStruct((2, n_tok, 2 * HD), BF16),
    )
    results = pl.pallas_call(
        fused,
        out_shape=outs,
        in_specs=[hbm, vmem, hbm, hbm, vmem, vmem, pl.BlockSpec(memory_space=pltpu.SMEM)],
        out_specs=(hbm, hbm),
        scratch_shapes=[
            pltpu.VMEM((8, 4, tok, kdim), BF16),
            pltpu.VMEM((kdim, n_q), BF16),
            pltpu.VMEM((kdim, n_q), BF16),
            pltpu.VMEM((4, n_kv, kdim), BF16),
            pltpu.VMEM((n_head, kdim), BF16),
            pltpu.VMEM((N_STEPS, 2, tok // 2, n_q), BF16),
            pltpu.VMEM((8, tok + 16, n_head), BF16),
            pltpu.VMEM((N_STEPS, 2, 3, tok // 2, n_q), BF16),
            pltpu.VMEM((4, 2, 3, tok + 16, n_head), BF16),
            pltpu.VMEM((8, 4, tok + 16, n_head), BF16),
            pltpu.VMEM((n_tok, 128), F32),
            pltpu.VMEM((n_tok, 128), F32),
            pltpu.VMEM((n_tok, 128), F32),
            dma((3,)),
            dma((2,)), dma((N_STEPS // 2,)), dma(()), dma((N_STEPS // 2,)),
            dma((2,)), dma((N_STEPS // 2,)), dma(()), dma((1,)),
            dma(()), dma((N_STEPS, 2)), dma(()), dma((4, 2)),
            dma(()), dma((2,)),
            pltpu.VMEM((n_tok, n_q), BF16),
            pltpu.VMEM((2, n_tok, 2 * HD), BF16),
            dma((2,)),
        ],
        compiler_params=pltpu.CompilerParams(
            collective_id=0, has_side_effects=True, vmem_limit_bytes=62 * 1024 * 1024
        ),
        name="fused",
    )(
        hidden_rows,
        norm_gain,
        w_query,
        w_keyval.T,
        positions.reshape(-1, 128),
        jnp.asarray(freq),
        keyval_order,
    )
    return pl.pallas_call(
        pass_on,
        out_shape=outs,
        in_specs=[hbm, hbm],
        out_specs=(hbm, hbm),
        scratch_shapes=[pltpu.VMEM(out.shape, out.dtype) for out in outs] + [dma((2, 2, 2))],
        name="pass_on",
    )(*results)


def solution(mesh):
    in_specs = (
        P(("gx", "gy"), "gz"),
        P("gz"),
        P("gz", ("gx", "gy")),
        P("gz", ("gx", "gy")),
        P("gz"),
        P(),
    )
    out_specs = (P("gz", ("gx", "gy")), P("gy", "gz", None))
    return jax.shard_map(body, mesh=mesh, in_specs=in_specs, out_specs=out_specs, check_vma=False)
```

```python
import functools
import math

import jax
import jax.numpy as jnp
import numpy as np
from jax import lax
from jax.experimental import pallas as pl
from jax.experimental.pallas import tpu as pltpu
from jax.sharding import PartitionSpec as P

D = 16384
KVH = 8
HD = 128
rope_base = 500000.0
norm_eps = 1e-05

MESH = pl.DeviceIdType.MESH
F32 = jnp.float32
BF16 = jnp.bfloat16

O, L, R, F = 0, 3, 1, 2

ARRIVALS = [
    [],
    [(L, O, 0), (R, O, 1)],
    [(L, O, 1), (R, O, 0)],
    [(O, L, 0), (O, R, 1), "weights_own"],
    [(F, O, 0), (F, O, 1)],
    [(L, L, 0), (R, R, 1)],
    [(O, L, 1), (O, R, 0)],
    ["weights_near", (L, R, 1), (R, L, 0)],
    [(L, L, 1), (R, R, 0)],
    [(L, R, 0), (R, L, 1)],
    ["weights_far", "kv_products", (F, L, 0), (F, R, 1)],
    [(O, F, 0), (O, F, 1)],
    ["kv_relay", (F, R, 0), (F, L, 1)],
    ["kv_plane", (L, F, 0), (R, F, 1)],
    ["kv_owner", (L, F, 1), (R, F, 0)],
    [(F, F, 0), (F, F, 1)],
]
STEPS = [(O, O, 0), (O, O, 1)] + [e for events in ARRIVALS for e in events if not isinstance(e, str)]
N_STEPS = len(STEPS)
PAIR = {step: n // 2 for n, step in enumerate(STEPS)}

def slot_counts(n):
    lag = 4 if n < 13 else 2
    return max(2 * n, 2), max(2 * n - lag, 0), max(2 * n - 2 * lag, 0)


SLOTS = [(events, *slot_counts(n)) for n, events in enumerate(ARRIVALS[:-1])] + [
    ([], 30, 26, 24),
    (ARRIVALS[-1], 30, 28, 26),
    (["kv_z"], 32, 30, 28),
    (["kv_far"], 32, 32, 30),
    (["kv_x", "owner_early"], 32, 32, 32),
]
KV_STEPS = (O, L, R, F)

KV_Z = [[(O, L, 0), (O, R, 1)], [(O, L, 1), (O, R, 0)]]
KV_FAR = [[(O, F, 0), (O, F, 1)], [(L, O, 0), (R, O, 1)]]
KV_X = [[(L, O, 1), (R, O, 0)], [(L, L, 0), (R, R, 1)], [(L, R, 0), (R, L, 1)]]
KV_LAST = [
    [(L, F, 0), (R, F, 1)], [(F, O, 0), (F, O, 1)], [(L, R, 1), (R, L, 0)], [(L, L, 1), (R, R, 0)],
    [(F, L, 0), (F, R, 1)], [(L, F, 1), (R, F, 0)], [(F, R, 0), (F, L, 1)], [(F, F, 0), (F, F, 1)],
]
EARLY = 24


def lookup(t, values):
    return sum((t == k).astype(jnp.int32) * v for k, v in enumerate(values) if v)


def fused(
    h_hbm, gain_ref, wq_hbm, wkv_hbm, pos_ref, freq_ref, order_ref,
    q_hbm, kv_hbm,
    rows, wq, w, wkv, w_kv, part, part_kv, inbox, inbox_kv, kvs, cosines, sines,
    load_sem, a_send, a_recv, a_side_send, a_side_recv,
    k_send, k_recv, k_side_send, k_side_recv, r_send, r_recv, r_kv_send, r_kv_recv,
    w_send, w_recv, q_ref, kv_ref, out_sem,
):
    gx, gy, gz = lax.axis_index("gx"), lax.axis_index("gy"), lax.axis_index("gz")
    x, core, zh = gx // 2, gx % 2, gy
    zl, y = gz // 4, gz % 4
    tok = rows.shape[2]
    part_tok = tok // 2
    kdim = rows.shape[3]
    n_q = wq.shape[1]
    n_kv = wkv.shape[1]
    n_head = 4 * n_kv

    def at(xx, cc, zz, yy, ll):
        return (2 * xx + cc, zz, ll * 4 + yy)

    sibling = at(x, 1 - core, zh, y, zl)
    x_up = at((x + 1) % 4, core, zh, y, zl)
    x_down = at((x + 3) % 4, core, zh, y, zl)
    z_up = at(x, core, (zh + 1) % 4, y, zl)
    z_down = at(x, core, (zh + 3) % 4, y, zl)

    loads = [
        pltpu.make_async_copy(h_hbm, rows.at[gx, gy], load_sem.at[0]),
        pltpu.make_async_copy(wq_hbm, wq, load_sem.at[1]),
        pltpu.make_async_copy(wkv_hbm, wkv.at[gy], load_sem.at[2]),
    ]
    loads[0].start()

    barrier = pltpu.get_barrier_semaphore()
    peers = [
        sibling, x_up, x_down, z_up, z_down,
        at(x, core, zh, (y + 1) % 4, zl), at(x, core, zh, (y + 3) % 4, zl), at(x, core, zh, y, 1 - zl),
    ]
    for peer in peers:
        pl.semaphore_signal(barrier, inc=1, device_id=peer, device_id_type=MESH)

    class Gather:
        def __init__(self, buf, sends, recv, side_send, side_recv):
            self.buf, self.sends, self.recv = buf, sends, recv
            self.side_send, self.side_recv = side_send, side_recv
            self.size, self.extra = tok // 2, buf.shape[2] - tok

        def piece(self, ox, oz, p, whole=False):
            size = self.size + (self.extra if whole and p else 0)
            return self.buf.at[2 * ((x + ox) % 4) + core, (zh + oz) % 4, pl.ds(p * self.size, size)]

        def push(self, ox, oz, p, to_x, to_z, target):
            along_z = to_x == O
            ref = self.piece(ox, oz, p, whole=along_z)
            pltpu.make_async_remote_copy(
                src_ref=ref, dst_ref=ref, send_sem=self.sends.at[int(along_z)],
                recv_sem=self.recv.at[PAIR[to_x, to_z, p]], device_id=target, device_id_type=MESH,
            ).start()

        def side(self, ox, oz, p):
            ref = self.piece(ox, oz, p)
            n = PAIR[ox, oz, p] if self.side_recv.shape[0] > 1 else 0
            pltpu.make_async_remote_copy(
                src_ref=ref, dst_ref=ref, send_sem=self.side_send, recv_sem=self.side_recv.at[n],
                device_id=sibling, device_id_type=MESH,
            ).start()

        def begin(self):
            for p in (0, 1):
                self.push(O, O, p, O, L, z_up)
                self.push(O, O, 1 - p, O, R, z_down)
                self.push(O, O, p, L, O, x_up)
                self.push(O, O, 1 - p, R, O, x_down)
            for p in (0, 1):
                self.side(O, O, p)

        def forward_z(self):
            self.push(O, L, 0, O, F, z_up)
            self.push(O, R, 1, O, F, z_down)

        def arrive(self, *pieces, late=False):
            whole = self.buf.at[0, 0] if pieces[0][0] == O else self.buf.at[0, 0, pl.ds(0, tok)]
            received(whole, self.recv.at[PAIR[pieces[0]]])
            if pieces[0] == (O, L, 0) and not late:
                self.forward_z()
            for ox, oz, p in pieces:
                if ox == O:
                    self.push(O, oz, p, L, oz, x_up)
                if (ox, p) == (L, 0):
                    self.push(L, oz, 0, F, oz, x_up)
            for ox, oz, p in pieces[::-1]:
                if ox == O:
                    self.push(O, oz, p, R, oz, x_down)
                if (ox, p) == (R, 1):
                    self.push(R, oz, 1, F, oz, x_down)
            for piece in pieces:
                self.side(*piece)

        def finish(self):
            left(self.buf.at[pl.ds(0, 8), pl.ds(0, 3), pl.ds(0, self.size)], self.sends.at[0])
            left(self.buf.at[0, pl.ds(0, 3)], self.sends.at[1])
            left(self.buf.at[:, :, pl.ds(0, self.size)], self.side_send)

    def received(ref, sem):
        pltpu.make_async_remote_copy(
            src_ref=ref, dst_ref=ref, send_sem=a_side_send, recv_sem=sem, device_id=sibling, device_id_type=MESH
        ).wait_recv()

    def left(ref, sem):
        pltpu.make_async_remote_copy(
            src_ref=ref, dst_ref=ref, send_sem=sem, recv_sem=a_recv.at[0], device_id=sibling, device_id_type=MESH
        ).wait_send()

    gather = Gather(rows, a_send, a_recv, a_side_send, a_side_recv)
    kv_gather = Gather(kvs, k_send, k_recv, k_side_send, k_side_recv)

    half_kv = n_kv // 2

    def weights_copy(oz, p, to_z, target):
        ref = wkv.at[(zh + oz) % 4, pl.ds(p * half_kv, half_kv)]
        return pltpu.make_async_remote_copy(
            src_ref=ref, dst_ref=ref, send_sem=w_send, recv_sem=w_recv.at[0 if (to_z, p) in ((L, 0), (R, 1)) else 1],
            device_id=target, device_id_type=MESH,
        )

    weights_sent = [
        (O, 0, L, z_up), (O, 1, R, z_down), (O, 1, L, z_up), (O, 0, R, z_down),
        (L, 0, F, z_up), (R, 1, F, z_down),
    ]

    def weights_own():
        for args in weights_sent[:4]:
            weights_copy(*args).start()

    def weights_near():
        received(wkv.at[0], w_recv.at[0])
        for args in weights_sent[4:]:
            weights_copy(*args).start()
        gather.forward_z()

    def weights_far():
        received(wkv.at[pl.ds(0, 2)], w_recv.at[1])
        for g in range(4):
            w_kv[g * n_kv : (g + 1) * n_kv, :] = (wkv[g].astype(F32) * gain_ref[...].astype(F32)[None, :]).astype(BF16)

    loads[0].wait()
    loads[1].start()
    loads[2].start()
    pl.semaphore_wait(barrier, len(peers))
    gather.begin()

    loads[1].wait()
    loads[2].wait()
    side_len = 128
    row_id = lax.broadcasted_iota(jnp.int32, (side_len, side_len), 0)
    lane = lax.broadcasted_iota(jnp.int32, (side_len, side_len), 1)

    for i in range(kdim // side_len):
        band = slice(i * side_len, (i + 1) * side_len)
        gain = jnp.broadcast_to(gain_ref[band].astype(F32)[None, :], (side_len, side_len))
        diagonal = jnp.where(row_id == lane, gain, 0.0).astype(BF16)
        w[band, 0:n_q] = jnp.dot(diagonal, wq[band, :], preferred_element_type=F32).astype(BF16)

    def tables(i, carry):
        spread = jnp.broadcast_to(pos_ref[pl.ds(i, 1), :].astype(F32), (side_len, side_len))
        angles = jnp.transpose(spread) * freq_ref[0:1, :]
        band = pl.ds(pl.multiple_of(i * side_len, side_len), side_len)
        cosines[band, :] = jnp.cos(angles)
        s = jnp.sin(angles)
        sines[band, :] = jnp.where(lane % 2 == 0, -s, s)
        return carry

    lax.fori_loop(0, pos_ref.shape[0], tables, 0)

    def unit(t, xx, c):
        y_own = (2 * xx + c) % 4
        zl_own = xx // 2
        step = 1 + 2 * ((t + c) % 2)
        relay, far, direct = (y_own + step) % 4, (y_own + 2) % 4, (y_own + 4 - step) % 4
        return y_own, zl_own, relay, far, direct

    class Reduction:
        def __init__(self, part, inbox, send, recv):
            self.part, self.inbox, self.send, self.recv = part, inbox, send, recv

        def copy(self, t, c, slot, target):
            return pltpu.make_async_remote_copy(
                src_ref=self.own(t, c), dst_ref=self.inbox.at[t, c, slot], send_sem=self.send,
                recv_sem=self.recv.at[t, c], device_id=target, device_id_type=MESH,
            )

        def landed(self, t, c, count):
            received(self.inbox.at[t, c, pl.ds(0, count)], self.recv.at[t, c])

        def total(self, t, c, slots, band, cols):
            value = self.own(t, c)[band, cols].astype(F32)
            for slot in slots:
                value = value + self.inbox[t, c, slot, band, cols].astype(F32)
            return value

        def first(self, t):
            for c in (0, 1):
                y_own, _, relay, far, direct = unit(t, self.place(t)[0], c)

                @pl.when(y == far)
                def _():
                    self.copy(t, c, 0, at(x, core, zh, relay, zl)).start()

                @pl.when(y == direct)
                def _():
                    self.copy(t, c, 0, at(x, core, zh, y_own, zl)).start()

        def relay(self, t):
            for c in (0, 1):
                y_own, _, relay, far, direct = unit(t, self.place(t)[0], c)

                @pl.when(y == relay)
                def _():
                    self.landed(t, c, 1)
                    self.add_up(t, c, [0])
                    self.copy(t, c, 1, at(x, core, zh, y_own, zl)).start()

        def plane(self, t):
            for c in (0, 1):
                y_own, zl_own, relay, far, direct = unit(t, self.place(t)[0], c)

                @pl.when((y == y_own) & (zl != zl_own))
                def _():
                    self.landed(t, c, 2)
                    self.add_up(t, c, [0, 1])
                    self.copy(t, c, 2, at(x, core, zh, y, zl_own)).start()

        def owner(self, t):
            for c in (0, 1):
                xx, zz = self.place(t)
                y_own, zl_own, relay, far, direct = unit(t, xx, c)

                @pl.when((y == y_own) & (zl == zl_own))
                def _():
                    self.landed(t, c, 3)
                    self.store(t, c, zz)

    tile_lane = lax.broadcasted_iota(jnp.int32, (tok, 128), 1)
    short_row = lax.broadcasted_iota(jnp.int32, (16, 128), 0)

    def rotate(tile, cos_t, sin_t):
        swapped = jnp.where(tile_lane[: tile.shape[0]] % 2 == 0, pltpu.roll(tile, 127, 1), pltpu.roll(tile, 1, 1))
        return tile * cos_t + swapped * sin_t

    class QueryReduction(Reduction):
        def place(self, t):
            return (x + lookup(t, [s[0] for s in STEPS])) % 4, (zh + lookup(t, [s[1] for s in STEPS])) % 4

        def own(self, t, c):
            return self.part.at[t, c]

        def rows_of(self, t):
            return lookup(t, [s[2] for s in STEPS]) * part_tok

        def add_up(self, t, c, slots):
            for n0 in range(0, n_q, 128):
                cols = slice(n0, n0 + 128)
                self.own(t, c)[:, cols] = self.total(t, c, slots, slice(None), cols).astype(BF16)

        def store(self, t, c, zz):
            band = pl.ds(pl.multiple_of(zz * tok + self.rows_of(t), part_tok), part_tok)
            cos_t, sin_t = cosines[band, :], sines[band, :]
            for n0 in range(0, n_q, 128):
                cols = slice(n0, n0 + 128)
                value = self.total(t, c, range(3), slice(None), cols)
                q_ref[band, cols] = rotate(value, cos_t, sin_t).astype(BF16)

    class KeyValueReduction(Reduction):
        def place(self, k):
            return (x + lookup(k, KV_STEPS)) % 4, zh

        def own(self, k, c):
            return self.part.at[2 * k + c]

        def add_up(self, t, c, slots):
            tile = self.total(t, c, slots, pl.ds(tok, 16), slice(0, 128))
            rest = tile - tile.astype(BF16).astype(F32)
            tile = jnp.where(short_row == 1, tile + pltpu.roll(rest, 1, 0), tile)
            self.own(t, c)[tok : tok + 16, 0:128] = tile.astype(BF16)
            for n0 in range(0, n_head, 128):
                cols = slice(n0, n0 + 128)
                self.own(t, c)[0:tok, cols] = self.total(t, c, slots, pl.ds(0, tok), cols).astype(BF16)

        def store(self, t, c, zz):
            band = pl.ds(pl.multiple_of(zz * tok, tok), tok)
            tile = self.total(t, c, range(3), pl.ds(tok, 16), slice(0, 128))
            square = jnp.sum(jnp.where(short_row < 2, tile, 0.0), axis=0, keepdims=True)
            factor = lax.rsqrt(square / D + norm_eps)
            first = factor.astype(BF16).astype(F32)
            second = (factor - first).astype(BF16).astype(F32)
            third = factor - first - second
            spread = jnp.where(short_row == 0, first, jnp.where(short_row == 1, second, third))
            kvs[gx, gy, tok : tok + 16, 0:128] = spread.astype(BF16)
            kvs[gx, gy, tok : tok + 16, 128:256] = jnp.zeros((16, 128), BF16)
            factor = jnp.transpose(jnp.broadcast_to(factor, (tok, 128)))
            everything = pl.ds(0, tok)
            key = self.total(t, c, range(3), everything, slice(0, 128)) * factor
            kvs[gx, gy, 0:tok, 0:128] = rotate(key, cosines[band, :], sines[band, :]).astype(BF16)
            value = self.total(t, c, range(3), everything, slice(128, 256)) * factor
            kvs[gx, gy, 0:tok, 128:256] = value.astype(BF16)

    query = QueryReduction(part, inbox, r_send, r_recv)
    keyval = KeyValueReduction(part_kv, inbox_kv, r_kv_send, r_kv_recv)

    def compute(t):
        xx, zz = query.place(t)
        p = lookup(t, [s[2] for s in STEPS])

        @pl.when(t % 2 == 0)
        def _():
            received(rows.at[0, 0], a_side_recv.at[t // 2])

        band = pl.ds(pl.multiple_of(p * part_tok, part_tok), part_tok)
        lhs = rows[pl.ds(2 * xx, 2), zz, band].reshape(tok, kdim)
        for n0 in range(0, n_q, 256):
            c_tile = jnp.dot(lhs, w[:, n0 : n0 + 256], preferred_element_type=F32).astype(BF16)
            part[t, 0, :, n0 : n0 + 256] = c_tile[:part_tok]
            part[t, 1, :, n0 : n0 + 256] = c_tile[part_tok:]
        query.first(t)

    def spread_factor(oz):
        zz = (zh + oz) % 4
        pieces = kvs[gx, zz, tok : tok + 16, 0:128].astype(F32)
        factor = jnp.sum(jnp.where(short_row < 3, pieces, 0.0), axis=0, keepdims=True)
        band = pl.ds(pl.multiple_of(zz * tok, tok), tok)
        factor = jnp.transpose(jnp.broadcast_to(factor, (tok, 128)))
        cosines[band, :] = cosines[band, :] * factor
        sines[band, :] = sines[band, :] * factor

    wide_lane = lax.broadcasted_iota(jnp.int32, (2 * tok, 128), 1)

    def kv_product(k):
        xx, zz = keyval.place(k)
        pair = pl.ds(2 * xx, 2)
        squares = jnp.zeros((2 * tok, 128), F32)
        for k0 in range(0, kdim, 128):
            some = rows[pair, zz, :, k0 : k0 + 128].reshape(2 * tok, 128).astype(F32)
            squares = squares + some * some
        square = jnp.sum(squares, axis=1, keepdims=True)
        high = square.astype(BF16).astype(F32)
        spread = jnp.where(wide_lane == 0, high, jnp.where(wide_lane == 1, square - high, 0.0))
        lhs = rows[pair, zz].reshape(2 * tok, kdim)
        tile = lax.dot_general(lhs, w_kv[...], (((1,), (1,)), ((), ())), preferred_element_type=F32).astype(BF16)
        for c in (0, 1):
            part_kv[2 * k + c, 0:tok, :] = tile[c * tok : (c + 1) * tok]
            turned = jnp.transpose(spread[c * tok : (c + 1) * tok])
            part_kv[2 * k + c, tok : tok + 16, 0:128] = turned[0:16].astype(BF16)
            part_kv[2 * k + c, tok : tok + 16, 128:256] = jnp.zeros((16, 128), BF16)
        keyval.first(k)

    def stages(stage, begin, end=N_STEPS):
        lax.fori_loop(begin, end, lambda t, carry: (stage(t), carry)[1], 0)

    named = {
        "kv_z": lambda: ([kv_gather.arrive(*pieces) for pieces in KV_Z], [spread_factor(oz) for oz in (O, L, R)]),
        "kv_far": lambda: ([kv_gather.arrive(*pieces) for pieces in KV_FAR], spread_factor(F)),
        "kv_x": lambda: [kv_gather.arrive(*pieces) for pieces in KV_X],
        "owner_early": lambda: stages(owner_early, 0, EARLY),
        "weights_near": weights_near,
        "weights_far": weights_far,
        "kv_products": lambda: stages(kv_product, 0, 4),
        "kv_relay": lambda: stages(keyval.relay, 0, 4),
        "kv_owner": lambda: (stages(keyval.owner, 0, 4), kv_gather.begin()),
        "kv_plane": lambda: stages(keyval.plane, 0, 4),
    }

    is_late = [int(s[1] == F) for s in STEPS[:EARLY]] + [1] * (N_STEPS - EARLY)

    def owner_early(t):
        @pl.when(lookup(t, is_late) == 0)
        def _():
            query.owner(t)

    def owner_late(t):
        @pl.when(lookup(t, is_late) == 1)
        def _():
            query.owner(t)

    def slot(n, carry):
        for k, (events, _, _, _) in enumerate(SLOTS):
            if events:

                @pl.when(n == k)
                def _():
                    for event in events:
                        if isinstance(event, str) and event != "weights_own":
                            named[event]()
                    pieces = [event for event in events if not isinstance(event, str)]
                    if pieces:
                        gather.arrive(*pieces, late=True)
                    if "weights_own" in events:
                        weights_own()

        for at_slot, stage in ((1, compute), (2, query.relay), (3, query.plane)):
            counts = [s[at_slot] for s in SLOTS]
            stages(stage, lookup(n, [0] + counts[:-1]), lookup(n, counts))
        return carry

    lax.fori_loop(0, len(SLOTS), slot, 0)

    def owner_near(t):
        @pl.when(lookup(t, [int(s[1] != F) for s in STEPS]) == 1)
        def _():
            query.owner(t)

    def owner_far(t):
        @pl.when(lookup(t, [int(s[1] == F) for s in STEPS[:28]] + [1] * 4) == 1)
        def _():
            query.owner(t)

    kv_gather.arrive(*KV_LAST[0])
    stages(owner_late, 0)
    q_out = pltpu.make_async_copy(q_ref, q_hbm, out_sem.at[0])
    q_out.start()
    for event in KV_LAST[1:]:
        kv_gather.arrive(*event)
    received(kvs.at[:, :, pl.ds(0, tok // 2)], k_side_recv.at[0])
    slots = kv_ref.shape[0]
    for s in range(slots):
        head = order_ref[slots * gy + s]
        for g in range(4):
            kv_ref[s, g * tok : (g + 1) * tok, :] = kvs[head, g, 0:tok, :]
    kv_out = pltpu.make_async_copy(kv_ref, kv_hbm, out_sem.at[1])
    kv_out.start()

    gather.finish()
    kv_gather.finish()

    left(wkv.at[pl.ds(0, 3)], w_send)
    owned = N_STEPS // 4
    left(part.at[pl.ds(0, N_STEPS - owned // 2)], r_send)
    left(part_kv.at[pl.ds(0, 7)], r_kv_send)
    q_out.wait()
    kv_out.wait()


def pass_on(q_in, kv_in, q_out, kv_out, q_buf, kv_buf, sems):
    takes, puts = [], []
    for n, (source, buf, target) in enumerate(((q_in, q_buf, q_out), (kv_in, kv_buf, kv_out))):
        half = buf.shape[0] // 2
        for i in (0, 1):
            piece = pl.ds(i * half, half)
            takes.append(pltpu.make_async_copy(source.at[piece], buf.at[piece], sems.at[0, n, i]))
            puts.append(pltpu.make_async_copy(buf.at[piece], target.at[piece], sems.at[1, n, i]))
    for take in takes:
        take.start()
    for take, put in zip(takes, puts):
        take.wait()
        put.start()
    for put in puts:
        put.wait()


def body(hidden_rows, norm_gain, w_query, w_keyval, positions, keyval_order):
    tok, kdim = hidden_rows.shape
    n_q, n_kv = w_query.shape[1], w_keyval.shape[1]
    n_head = 4 * n_kv
    n_tok = positions.shape[0]
    freq = np.exp((np.arange(128) // 2) * (-2.0 * math.log(rope_base) / HD)).astype(np.float32)[None, :]
    hbm = pl.BlockSpec(memory_space=pl.ANY)
    vmem = pl.BlockSpec(memory_space=pltpu.VMEM)
    dma = pltpu.SemaphoreType.DMA
    outs = (
        jax.ShapeDtypeStruct((n_tok, n_q), BF16),
        jax.ShapeDtypeStruct((2, n_tok, 2 * HD), BF16),
    )
    results = pl.pallas_call(
        fused,
        out_shape=outs,
        in_specs=[hbm, vmem, hbm, hbm, vmem, vmem, pl.BlockSpec(memory_space=pltpu.SMEM)],
        out_specs=(hbm, hbm),
        scratch_shapes=[
            pltpu.VMEM((8, 4, tok, kdim), BF16),
            pltpu.VMEM((kdim, n_q), BF16),
            pltpu.VMEM((kdim, n_q), BF16),
            pltpu.VMEM((4, n_kv, kdim), BF16),
            pltpu.VMEM((n_head, kdim), BF16),
            pltpu.VMEM((N_STEPS, 2, tok // 2, n_q), BF16),
            pltpu.VMEM((8, tok + 16, n_head), BF16),
            pltpu.VMEM((N_STEPS, 2, 3, tok // 2, n_q), BF16),
            pltpu.VMEM((4, 2, 3, tok + 16, n_head), BF16),
            pltpu.VMEM((8, 4, tok + 16, n_head), BF16),
            pltpu.VMEM((n_tok, 128), F32),
            pltpu.VMEM((n_tok, 128), F32),
            dma((3,)),
            dma((2,)), dma((N_STEPS // 2,)), dma(()), dma((N_STEPS // 2,)),
            dma((2,)), dma((N_STEPS // 2,)), dma(()), dma((1,)),
            dma(()), dma((N_STEPS, 2)), dma(()), dma((4, 2)),
            dma(()), dma((2,)),
            pltpu.VMEM((n_tok, n_q), BF16),
            pltpu.VMEM((2, n_tok, 2 * HD), BF16),
            dma((2,)),
        ],
        compiler_params=pltpu.CompilerParams(
            collective_id=0, has_side_effects=True, vmem_limit_bytes=62 * 1024 * 1024
        ),
        name="fused",
    )(
        hidden_rows,
        norm_gain,
        w_query,
        w_keyval.T,
        positions.reshape(-1, 128),
        jnp.asarray(freq),
        keyval_order,
    )
    return pl.pallas_call(
        pass_on,
        out_shape=outs,
        in_specs=[hbm, hbm],
        out_specs=(hbm, hbm),
        scratch_shapes=[pltpu.VMEM(out.shape, out.dtype) for out in outs] + [dma((2, 2, 2))],
        name="pass_on",
    )(*results)


def solution(mesh):
    in_specs = (
        P(("gx", "gy"), "gz"),
        P("gz"),
        P("gz", ("gx", "gy")),
        P("gz", ("gx", "gy")),
        P("gz"),
        P(),
    )
    out_specs = (P("gz", ("gx", "gy")), P("gy", "gz", None))
    return jax.shard_map(body, mesh=mesh, in_specs=in_specs, out_specs=out_specs, check_vma=False)
```
